256 devices in a mesh: parts: 2 (over z), genes: 64 (over x, y), samples: 2 (over core).
Axes of the slice: x: 8, y: 8, z: 2, core: 2. Of those that a mesh axis runs over, the one named last changes fastest.
The devices are a block of a 8x8x16 slice.
Arguments:
- dosage: bfloat16 [262144, 2048], P(('parts', 'genes'), 'samples'), parts along dimension 0, may hold values from -6 to 6
- expression: bfloat16 [1024, 2048], P(('parts', 'genes'), 'samples'), parts along dimension 0, may hold values from -6 to 6
- intron_counts: bfloat16 [4096, 20480], P(('parts', 'samples', 'genes')), parts along dimension 0, may hold values from 1 to 100
- cluster_sizes: int32 [1024, 8], P('parts'), parts along dimension 0, may hold values from 1 to 12, 40 in all within a row
- valid_mask: int32 [1024, 40], P('parts'), parts along dimension 0, may hold values 0 or 1
- gene_block: int32 [1024], P('parts'), parts along dimension 0, may hold values from 0 to 511, each once
- window_start: int32 [1024], P(('parts', 'genes')), parts along dimension 0, may hold values from 0 to 1024, as said below
Outputs:
- assoc: bfloat16 [1024, 41, 2048], P(('parts', 'genes'), None, 'samples'), parts along dimension 0
The draws below stay inside these ranges and needn't reach their ends.
There are 2 independent parts, one for each index of `parts`. The reference program is written for one: setup_inputs(seed, part) draws one part's arguments, and reference() takes and returns one part's arrays. A program takes and returns all parts, laid end to end along the dimension named above; each array names one. Nothing has to cross between parts.
Inputs may be any that keep to these rules, and one draw needn't show every extreme that they name: Every window_start is a multiple of 128 and at most 1024; some gene reaches 1024 in every draw. `gene_block`: a permutation of the genes. `cluster_sizes`: each row sums to 40.
All inputs are finite; a program needn't handle non-finite values.
Results may differ from the reference program's by a relative error of at most 0.0058.
Values may be sent and summed in bfloat16 or wider, within the bound.
A program may use at most 64 MiB of HBM per device.

```python
import math
import jax
import jax.numpy as jnp
import numpy as np
from jax import lax

GENE_DEV = 8
W = 2048
SLOTS = 40
CLUST = 8
CL_MOST = 12
SPILL = 1024
ALIGN = 128
PHEN = 41
GENES = 512
SAMP = 2048
VARIANTS = 131072
INTRONS = 20480
N_GENES = 64


def draw_window_start(key, part):
    draw_starts, draw_pick = jax.random.split(jax.random.fold_in(key, 7))
    starts = jax.random.randint(draw_starts, (GENES,), 0, SPILL // ALIGN + 1, dtype=jnp.int32) * ALIGN
    chosen = jax.random.randint(draw_pick, (), 0, GENES, dtype=jnp.int32)
    return jnp.where(jnp.arange(GENES, dtype=jnp.int32) == chosen, SPILL, starts).astype(jnp.int32)


def plant(array, key, least, high):
    spot = [jax.random.randint(jax.random.fold_in(key, axis), (), 0, length) for axis, length in enumerate(array.shape)]
    main_axis = array.shape.index(max(array.shape))
    neighbour = spot[:main_axis] + [(spot[main_axis] + 1) % array.shape[main_axis]] + spot[main_axis + 1:]
    return array.at[tuple(spot)].set(least).at[tuple(neighbour)].set(high)


def steps_of(own_key, shape, cuts, least, high):
    def one(dim, parts):
        heights = jax.random.uniform(jax.random.fold_in(jax.random.fold_in(own_key, 6), dim), (parts,), jnp.float32, least / len(cuts), high / len(cuts))
        return jnp.repeat(jnp.exp(heights), shape[dim] // parts).reshape((-1,) + (1,) * (len(shape) - dim - 1))

    factor_of = one(*cuts[0])
    for cut in cuts[1:]:
        factor_of = factor_of * one(*cut)
    return factor_of


def split_up(amount, total, most, lean):
    loads = [(1 << 20) // math.isqrt(rank ** lean) + 1 for rank in range(2, amount + 1)]
    spare, given = total - most - (amount - 1), [1] * (amount - 1)
    while spare > 0:
        movable = [i for i in range(amount - 1) if given[i] < most]
        mass, left = sum([loads[i] for i in movable]), spare
        for i in movable:
            more = min(most - given[i], max(1, left * loads[i] // mass), spare)
            given[i] = given[i] + more
            spare = spare - more
    return np.array([most] + given)


def uneven(key, count, total, bound, slope):
    if count == 2:
        one = jax.random.randint(key, (), max(1, total - bound), min(bound, total - 1) + 1)
        return jnp.stack([one, total - one])
    sizes = jnp.asarray(split_up(count, total, bound, slope), jnp.int32)
    couples = (count - 1) // 2
    giver, taker = sizes[1:1 + 2 * couples:2], sizes[2:2 + 2 * couples:2]
    slack = jnp.minimum(giver - 1, bound - taker)
    passed = jax.random.randint(jax.random.fold_in(key, 1), (couples,), 0, 1 << 20) % (slack + 1)
    sizes = sizes.at[1:1 + 2 * couples:2].set(giver - passed).at[2:2 + 2 * couples:2].set(taker + passed)
    return sizes[jax.random.permutation(jax.random.fold_in(key, 2), count)]


def scatter_about(own_key, shape, scale, bound, shards=(), held_as=jnp.bfloat16):
    entries = scale * jax.random.normal(own_key, shape, jnp.float32)
    if shards:
        entries = entries * steps_of(own_key, shape, shards, -0.22, 0.18)
    return jnp.clip(entries, -bound, bound).astype(held_as)


def setup_inputs(seed: int = 0, part: int = 0) -> dict:
    splits = jax.random.split(jax.random.key(seed), 8)
    own_keys = jax.random.split(jax.random.fold_in(splits[7], part), 8)
    dosage = scatter_about(own_keys[0], (VARIANTS, SAMP), 1.0, 6.0, ((0, 64), (1, 2)))
    expression = scatter_about(own_keys[1], (GENES, SAMP), 1.0, 6.0, ((0, 64), (1, 2)))
    intron_counts = jnp.clip(jnp.exp(math.log(100.0) - 4.6051702 * jax.random.uniform(own_keys[2], (SAMP, INTRONS), jnp.float32) ** steps_of(own_keys[2], (SAMP, INTRONS), ((0, 128),), -0.2, 0.2)), 1.0, 100.0).astype(jnp.bfloat16)
    cluster_sizes = jax.vmap(lambda own: uneven(own, CLUST, SLOTS, CL_MOST, 2))(jax.random.split(own_keys[3], GENES)).reshape((GENES, CLUST)).astype(jnp.int32)
    valid_mask = plant((jax.random.randint(own_keys[4], (GENES, SLOTS), 0, 4) < 3).astype(jnp.int32), jax.random.fold_in(own_keys[4], 1), 0, 1)
    gene_block = jax.random.permutation(own_keys[5], GENES).astype(jnp.int32)
    window_start = draw_window_start(jax.random.fold_in(jax.random.fold_in(splits[7], part), 71), part)
    return dict(dosage=dosage, expression=expression, intron_counts=intron_counts, cluster_sizes=cluster_sizes, valid_mask=valid_mask, gene_block=gene_block, window_start=window_start)


def cluster_ratios(counts, cluster_sizes, valid_mask):
    cluster_ends = jnp.cumsum(cluster_sizes, axis=1, dtype=jnp.int32)
    slot_index = jnp.arange(SLOTS, dtype=jnp.int32)
    cluster_id = lax.optimization_barrier(jnp.sum((cluster_ends[:, None, :] <= slot_index[None, :, None]).astype(jnp.int32), axis=2, dtype=jnp.int32))
    same_cluster = (cluster_id[:, :, None] == cluster_id[:, None, :]).astype(jnp.float32)
    live_counts = counts * valid_mask.astype(jnp.float32)[None, :, :]
    cluster_total = jnp.einsum('sgj,gjk->sgk', live_counts, same_cluster, precision=lax.Precision.HIGHEST)
    return (live_counts / jnp.maximum(cluster_total, 1.0)).astype(jnp.bfloat16)

def tile_window(owner_block, offset, width):
    leading = owner_block.shape[:-1]
    tiles = owner_block.reshape(leading + (owner_block.shape[-1] // ALIGN, ALIGN))
    first_tile = (offset // ALIGN).astype(jnp.int32)
    piece = lax.dynamic_slice_in_dim(tiles, first_tile, width // ALIGN, len(leading))
    return piece.reshape(leading + (width,))

def window_slices(product, row_sum, row_square, starts):

    def window_of(owner_block, offset):
        return tile_window(owner_block, offset, W)
    cross_part = jax.vmap(window_of, in_axes=(0, 0))(product, starts)
    sum_part = jax.vmap(window_of, in_axes=(None, 0))(row_sum, starts)
    square_part = jax.vmap(window_of, in_axes=(None, 0))(row_square, starts)
    return (cross_part, sum_part, square_part)

def finish_stats(cross_part, sum_part, square_part, phen_sum, phen_square, sample_count):
    numerator = cross_part - sum_part[:, None, :] * phen_sum[:, :, None] / sample_count
    dose_var = jnp.maximum(square_part - sum_part * sum_part / sample_count, 1.0)
    pheno_var = jnp.maximum(phen_square - phen_sum * phen_sum / sample_count, 1.0)
    return (numerator * lax.rsqrt(dose_var)[:, None, :] * lax.rsqrt(pheno_var)[:, :, None]).astype(jnp.bfloat16)

def reference(dosage, expression, intron_counts, cluster_sizes, valid_mask, gene_block, window_start):
    padded = jnp.concatenate([dosage, jnp.zeros((SPILL, SAMP), jnp.bfloat16)], axis=0)
    stored = intron_counts.reshape(SAMP, GENES, SLOTS)

    def owner_stats(owner_index):
        gene_ids = owner_index * GENE_DEV + jnp.arange(GENE_DEV, dtype=jnp.int32)
        dose_rows = lax.dynamic_slice_in_dim(padded, owner_index * W, W + SPILL, 0)
        counts = jnp.take(stored, gene_block[gene_ids], axis=1).astype(jnp.float32)
        ratios = cluster_ratios(counts, cluster_sizes[gene_ids], valid_mask[gene_ids])
        expr_rows = lax.dynamic_slice_in_dim(expression, owner_index * GENE_DEV, GENE_DEV, 0)
        pheno_panel = jnp.concatenate([expr_rows.T[:, :, None], ratios], axis=2).reshape(SAMP, GENE_DEV * PHEN)
        product = lax.dot_general(pheno_panel, dose_rows, (((0,), (1,)), ((), ())), preferred_element_type=jnp.float32)
        product = product.reshape(GENE_DEV, PHEN, W + SPILL)
        dose_float = dose_rows.astype(jnp.float32)
        row_sum = lax.optimization_barrier(jnp.sum(dose_float, axis=1))
        row_square = lax.optimization_barrier(jnp.sum(dose_float * dose_float, axis=1))
        pheno_float = pheno_panel.astype(jnp.float32)
        phen_sum = lax.optimization_barrier(jnp.sum(pheno_float, axis=0)).reshape(GENE_DEV, PHEN)
        phen_square = lax.optimization_barrier(jnp.sum(pheno_float * pheno_float, axis=0)).reshape(GENE_DEV, PHEN)
        cross_part, sum_part, square_part = window_slices(product, row_sum, row_square, window_start[gene_ids])
        return finish_stats(cross_part, sum_part, square_part, phen_sum, phen_square, float(SAMP))
    result = lax.map(owner_stats, jnp.arange(N_GENES, dtype=jnp.int32))
    return result.reshape(GENES, PHEN, W)
```

```python
import functools

import jax
import jax.numpy as jnp
from jax import lax
from jax.experimental import pallas as pl
from jax.experimental.pallas import tpu as pltpu
from jax.sharding import PartitionSpec as P

W = 2048
HALF = 1024
SLOTS = 40
ALIGN = 128
PHEN = 41
ROWS = 48
GENE_DEV = 8
LANES = 384
SIDE = 8
MESH = pl.DeviceIdType.MESH
NT = (((1,), (1,)), ((), ()))


def permuted(counts_ref, block_ref, msgs_ref, owner):
    lane = lax.broadcasted_iota(jnp.int32, (16, ALIGN), 1)
    last = counts_ref.shape[1] // ALIGN - 2
    tiles = [jnp.zeros((16, ALIGN), jnp.float32) for _ in range(3)]
    for j in range(GENE_DEV):
        first = block_ref[owner * GENE_DEV + j] * SLOTS
        tile = jnp.minimum(first // ALIGN, last)
        start = first - tile * ALIGN
        at = pl.multiple_of(tile * ALIGN, ALIGN)
        a = counts_ref[:, pl.ds(at, ALIGN)].astype(jnp.float32)
        b = counts_ref[:, pl.ds(pl.multiple_of(at + ALIGN, ALIGN), ALIGN)].astype(jnp.float32)
        q = j * SLOTS % ALIGN
        turn = (q - start + 2 * ALIGN) % ALIGN
        a = pltpu.roll(a, turn, 1)
        b = pltpu.roll(b, turn, 1)
        index = (lane - q + ALIGN) % ALIGN
        gene = jnp.where(index + start < ALIGN, a, b)
        t = j * SLOTS // ALIGN
        tiles[t] = jnp.where((lane >= q) & (lane < q + SLOTS), gene, tiles[t])
        if q + SLOTS > ALIGN:
            tiles[t + 1] = jnp.where(lane < q + SLOTS - ALIGN, gene, tiles[t + 1])
    msgs_ref[owner] = jnp.concatenate(tiles, axis=1).astype(jnp.bfloat16)


def permute(block_ref, counts_ref, msgs_ref):
    @pl.loop(0, msgs_ref.shape[0])
    def _(owner):
        permuted(counts_ref, block_ref, msgs_ref, owner)


def kernel(
    n,
    msgs,
    expr_ref,
    keyl_ref,
    idxl_ref,
    keyr_ref,
    idxr_ref,
    dose_ref,
    z_ref,
    raw,
    expr,
    panel,
    dose,
    stat,
    pstat,
    sd,
    back,
    direct_sem,
    relay_sem,
    panel_sem,
    sent_sem,
    local_sem,
    dose_sem,
    expr_sem,
    back_sem,
):
    me = lax.axis_index("genes")
    core = lax.axis_index("samples")
    x, y = me // SIDE, me % SIDE
    nxt, prv = (me + 1) % n, (me + n - 1) % n
    other = 1 - core
    xp = jnp.where(y > 0, x, (x + SIDE - 1) % SIDE)

    mine = pltpu.make_async_copy(dose_ref, dose.at[0], local_sem)
    mine.start()
    barrier = pltpu.get_barrier_semaphore()

    @pl.loop(1, n)
    def _(step):
        pl.semaphore_signal(
            barrier, inc=1, device_id={"genes": (me + step) % n}, device_id_type=MESH
        )

    pl.semaphore_signal(barrier, inc=1, device_id={"samples": other}, device_id_type=MESH)

    def send_chunk(dx):
        @pl.loop(0, SIDE)
        def _(yo):
            owner = ((x + dx) % SIDE) * SIDE + yo
            near = (yo - y + SIDE) % SIDE < SIDE // 2
            kind = jnp.where(near, 0, 1)
            dest = jnp.where(near, owner, (owner + 1) % n)

            @pl.when(dest != me)
            def _():
                pltpu.make_async_remote_copy(
                    src_ref=msgs.at[owner],
                    dst_ref=raw.at[kind, me],
                    send_sem=sent_sem.at[0],
                    recv_sem=direct_sem.at[kind, dx],
                    device_id={"genes": dest},
                    device_id_type=MESH,
                ).start()

            @pl.when(dest == me)
            def _():
                pltpu.make_async_copy(
                    msgs.at[owner], raw.at[kind, me], direct_sem.at[kind, dx]
                ).start()

    pl.semaphore_wait(barrier, n)

    @pl.loop(0, SIDE)
    def _(dx):
        send_chunk(dx)

    dose_copy = pltpu.make_async_remote_copy(
        src_ref=dose_ref,
        dst_ref=dose.at[1],
        send_sem=dose_sem.at[0],
        recv_sem=dose_sem.at[1],
        device_id={"samples": other},
        device_id_type=MESH,
    )
    dose_copy.start()
    expr_copy = pltpu.make_async_remote_copy(
        src_ref=expr_ref,
        dst_ref=expr.at[1],
        send_sem=expr_sem.at[0],
        recv_sem=expr_sem.at[1],
        device_id={"genes": nxt},
        device_id_type=MESH,
    )
    expr_copy.start()

    expr[0] = expr_ref[...]
    for kind in range(2):
        total = (keyr_ref[kind] == keyl_ref[kind]).astype(jnp.float32)
        live = (idxr_ref[...] == idxl_ref[kind]).astype(jnp.float32)
        sd[kind, : GENE_DEV * ROWS] = total.astype(jnp.bfloat16)
        sd[kind, GENE_DEV * ROWS :] = live.astype(jnp.bfloat16)
    expr_copy.wait()
    mine.wait()

    ones = jnp.ones((8, ALIGN), jnp.float32)

    def dose_stats(slot, first, rows):
        @pl.loop(0, rows // ALIGN)
        def _(r):
            at = pl.multiple_of(first + r * ALIGN, ALIGN)
            total = jnp.zeros((ALIGN, ALIGN), jnp.float32)
            square = jnp.zeros((ALIGN, ALIGN), jnp.float32)
            for k in range(HALF // ALIGN):
                value = dose[slot, pl.ds(at, ALIGN), k * ALIGN : (k + 1) * ALIGN].astype(jnp.float32)
                total = total + value
                square = square + value * value
            for which, part in enumerate((total, square)):
                stat[slot, which, :, pl.ds(at, ALIGN)] = lax.dot_general(
                    ones,
                    part,
                    NT,
                    precision=lax.Precision.HIGHEST,
                    preferred_element_type=jnp.float32,
                )

    def relay_chunk(dx):
        for kind in range(2):
            pltpu.make_async_copy(
                raw.at[kind, 0 : SIDE // 2], raw.at[kind, 0 : SIDE // 2], direct_sem.at[kind, dx]
            ).wait()
        for kind, partner in ((0, nxt), (1, prv)):
            xs = ((x if kind == 0 else xp) + SIDE - dx) % SIDE

            @pl.loop(0, SIDE // 2)
            def _(t):
                ys = (y + SIDE - t) % SIDE if kind == 0 else (y + t) % SIDE
                source = xs * SIDE + ys
                pltpu.make_async_remote_copy(
                    src_ref=raw.at[kind, source],
                    dst_ref=raw.at[1 - kind, source],
                    send_sem=sent_sem.at[1],
                    recv_sem=relay_sem.at[1 - kind, dx],
                    device_id={"genes": partner},
                    device_id_type=MESH,
                ).start()

    def ratio_chunk(dx):
        for kind in range(2):
            pltpu.make_async_copy(
                raw.at[kind, 0 : SIDE // 2], raw.at[kind, 0 : SIDE // 2], relay_sem.at[kind, dx]
            ).wait()
            xs = ((x if kind == 0 else xp) + SIDE - dx) % SIDE
            counts = raw[kind, pl.ds(xs * SIDE, SIDE)].reshape(ALIGN, LANES)
            both = lax.dot_general(sd[kind], counts, NT, preferred_element_type=jnp.float32)
            total, live = both[: GENE_DEV * ROWS], both[GENE_DEV * ROWS :]
            ratio = live / jnp.maximum(total, 1.0)
            own = expr[kind, :, pl.ds(pl.multiple_of(xs * ALIGN, ALIGN), ALIGN)].astype(jnp.float32)
            row = lax.broadcasted_iota(jnp.int32, (8, ALIGN), 0)
            for g in range(GENE_DEV):
                block = ratio[g * ROWS : (g + 1) * ROWS]
                head = jnp.where(row == 0, own[g : g + 1], block[:8])
                panel[kind, 0, xs, g * ROWS : (g + 1) * ROWS] = jnp.concatenate(
                    [head, block[8:]], axis=0
                ).astype(jnp.bfloat16)

    def panel_copy(kind, dx):
        xs = ((x if kind == 0 else xp) + SIDE - dx) % SIDE
        return pltpu.make_async_remote_copy(
            src_ref=panel.at[kind, 0, xs],
            dst_ref=panel.at[kind, 1, xs],
            send_sem=panel_sem.at[kind, 0],
            recv_sem=panel_sem.at[kind, 1],
            device_id={"samples": other},
            device_id_type=MESH,
        )

    def panel_chunk(dx):
        panel_copy(0, dx).start()

        @pl.when(core == 0)
        def _():
            panel_copy(1, dx).start()

    @pl.loop(0, SIDE // 2)
    def _(dx):
        dose_stats(0, dx * 512, 512)
        relay_chunk(dx)

    dose_copy.wait_recv()

    @pl.loop(0, SIDE // 2)
    def _(dx):
        dose_stats(1, dx * 512, 512)
        relay_chunk(SIDE // 2 + dx)

    ratio_chunk(0)

    @pl.loop(1, SIDE)
    def _(dx):
        ratio_chunk(dx)
        panel_chunk(dx - 1)

    panel_chunk(SIDE - 1)

    count = float(2 * HALF)
    for c in range(W // 512):
        at = slice(c * 512, (c + 1) * 512)
        total = stat[0, 0, :, at] + stat[1, 0, :, at]
        square = stat[0, 1, :, at] + stat[1, 1, :, at]
        stat[0, 0, :, at] = total * (1.0 / count)
        stat[0, 1, :, at] = lax.rsqrt(jnp.maximum(square - total * total / count, 1.0))

    def panel_wait(kind, way):
        pltpu.make_async_copy(panel.at[kind, 1], panel.at[kind, 1], panel_sem.at[kind, way]).wait()

    panel_wait(0, 1)

    @pl.when(core == 1)
    def _():
        panel_wait(1, 1)

    def pheno_stats(kind):
        for g in range(GENE_DEV):
            rows = slice(g * ROWS, (g + 1) * ROWS)
            total = jnp.zeros((ROWS, ALIGN), jnp.float32)
            square = jnp.zeros((ROWS, ALIGN), jnp.float32)
            for slot in range(2):
                for k in range(SIDE):
                    value = panel[kind, slot, k, rows].astype(jnp.float32)
                    total = total + value
                    square = square + value * value
            total = jnp.sum(total, axis=1, keepdims=True)
            square = jnp.sum(square, axis=1, keepdims=True)
            pstat[0, rows] = jnp.broadcast_to(total, (ROWS, ALIGN))
            scale = lax.rsqrt(jnp.maximum(square - total * total / count, 1.0))
            pstat[1, rows] = jnp.broadcast_to(scale, (ROWS, ALIGN))

    STEP = 256

    def assoc(kind, first, out_ref, scale):
        left = [
            jnp.concatenate([panel[kind, slot, k] for k in range(SIDE)], axis=1) for slot in range(2)
        ]

        @pl.loop(0, HALF // STEP)
        def _(c):
            at = pl.multiple_of(first + c * STEP, STEP)
            product = sum(
                lax.dot_general(
                    left[slot], dose[slot, pl.ds(at, STEP)], NT, preferred_element_type=jnp.float32
                )
                for slot in range(2)
            )
            for k in range(STEP // ALIGN):
                here = pl.ds(pl.multiple_of(at + k * ALIGN, ALIGN), ALIGN)
                mean = stat[0, 0, 0:1, here]
                dev = stat[0, 1, 0:1, here] * scale
                part = product[:, k * ALIGN : (k + 1) * ALIGN]
                part = (part - pstat[0] * mean) * dev * pstat[1]
                to = pl.ds(pl.multiple_of(c * STEP + k * ALIGN, ALIGN), ALIGN)
                out_ref[:, to] = part.astype(jnp.bfloat16)

    keep = jnp.where(me == 0, 0.0, 1.0)

    @pl.when(core == 0)
    def _():
        pheno_stats(0)
        assoc(0, 0, z_ref.at[0], 1.0)
        assoc(0, HALF, z_ref.at[1], 1.0)

    @pl.when(core == 1)
    def _():
        give = pltpu.make_async_remote_copy(
            src_ref=back,
            dst_ref=z_ref.at[1],
            send_sem=back_sem.at[0],
            recv_sem=back_sem.at[1],
            device_id={"genes": prv},
            device_id_type=MESH,
        )
        pheno_stats(1)
        assoc(1, 0, back, keep)
        give.start()
        pheno_stats(0)
        assoc(0, HALF, z_ref.at[0], 1.0)
        give.wait()

    dose_copy.wait_send()
    pltpu.make_async_copy(raw.at[0, 0 : n - 2], raw.at[0, 0 : n - 2], sent_sem.at[0]).wait()
    pltpu.make_async_copy(raw.at[0], raw.at[0], sent_sem.at[1]).wait()
    panel_wait(0, 0)

    @pl.when(core == 0)
    def _():
        panel_wait(1, 0)


def cut(start_ref, z_ref, out_ref):
    for g in range(GENE_DEV):
        first = start_ref[g] // ALIGN
        for m in range(HALF // ALIGN):
            t = first + m
            part = z_ref[
                t // SIDE, g * ROWS : (g + 1) * ROWS, pl.ds(pl.multiple_of(t % SIDE * ALIGN, ALIGN), ALIGN)
            ]
            out_ref[g, :, m * ALIGN : (m + 1) * ALIGN] = part[:PHEN]


def keys(sizes, mask):
    until = jnp.arange(8)[:, None] <= jnp.arange(8)[None, :]
    ends = jnp.sum(jnp.where(until, sizes[:, :, None], 0), axis=1)
    slot = jnp.arange(SLOTS, dtype=jnp.int32)
    cluster = jnp.sum((ends[:, None, :] <= slot[None, :, None]).astype(jnp.int32), axis=2)
    gene = jnp.arange(GENE_DEV, dtype=jnp.int32)[:, None]
    key = gene * 16 + cluster
    lane_key = jnp.where(mask > 0, key, -1).reshape(1, GENE_DEV * SLOTS)
    lane_key = jnp.pad(lane_key, ((0, 0), (0, LANES - GENE_DEV * SLOTS)), constant_values=-1)
    lane_idx = jnp.where(mask > 0, gene * SLOTS + slot[None], -1).reshape(1, GENE_DEV * SLOTS)
    lane_idx = jnp.pad(lane_idx, ((0, 0), (0, LANES - GENE_DEV * SLOTS)), constant_values=-1)
    row_key = jnp.pad(key, ((0, 0), (1, ROWS - PHEN)), constant_values=-2)
    return lane_key, lane_idx, row_key.reshape(GENE_DEV * ROWS, 1)


def shards(dosage, expression, intron_counts, cluster_sizes, valid_mask, gene_block, window_start):
    n = lax.axis_size("genes")
    me = lax.axis_index("genes")
    prv = (me + n - 1) % n
    lane_key, lane_idx, row_key = zip(
        *(
            keys(
                lax.dynamic_slice_in_dim(cluster_sizes, i * GENE_DEV, GENE_DEV, 0),
                lax.dynamic_slice_in_dim(valid_mask, i * GENE_DEV, GENE_DEV, 0),
            )
            for i in (me, prv)
        )
    )
    row_idx = jnp.arange(GENE_DEV, dtype=jnp.int32)[:, None] * SLOTS + jnp.arange(SLOTS, dtype=jnp.int32)[None]
    row_idx = jnp.pad(row_idx, ((0, 0), (1, ROWS - PHEN)), constant_values=-2).reshape(GENE_DEV * ROWS, 1)
    vmem = pl.BlockSpec(memory_space=pltpu.VMEM)
    smem = pl.BlockSpec(memory_space=pltpu.SMEM)
    dma = pltpu.SemaphoreType.DMA
    bf16, f32 = jnp.bfloat16, jnp.float32
    rows = GENE_DEV * ROWS
    msgs = pl.pallas_call(
        permute,
        out_shape=jax.ShapeDtypeStruct((n, 16, LANES), bf16),
        in_specs=[smem, vmem],
        out_specs=vmem,
        name="permute",
    )(gene_block, intron_counts)
    z = pl.pallas_call(
        functools.partial(kernel, n),
        out_shape=jax.ShapeDtypeStruct((2, rows, HALF), bf16),
        in_specs=[vmem, vmem, vmem, vmem, vmem, vmem, pl.BlockSpec(memory_space=pl.ANY)],
        out_specs=vmem,
        scratch_shapes=[
            pltpu.VMEM((2, n, 16, LANES), bf16),
            pltpu.VMEM((2, GENE_DEV, HALF), bf16),
            pltpu.VMEM((2, 2, SIDE, rows, ALIGN), bf16),
            pltpu.VMEM((2, W, HALF), bf16),
            pltpu.VMEM((2, 2, 8, W), f32),
            pltpu.VMEM((2, rows, ALIGN), f32),
            pltpu.VMEM((2, 2 * rows, LANES), bf16),
            pltpu.VMEM((rows, HALF), bf16),
            dma((2, SIDE)),
            dma((2, SIDE)),
            dma((2, 2)),
            dma((2,)),
            dma,
            dma((2,)),
            dma((2,)),
            dma((2,)),
        ],
        compiler_params=pltpu.CompilerParams(collective_id=0, has_side_effects=True),
        name="associate",
    )(
        msgs,
        expression,
        jnp.stack(lane_key),
        jnp.stack(lane_idx),
        jnp.stack(row_key),
        row_idx,
        dosage,
    )
    return pl.pallas_call(
        cut,
        out_shape=jax.ShapeDtypeStruct((GENE_DEV, PHEN, HALF), bf16),
        in_specs=[smem, vmem],
        out_specs=vmem,
        name="cut",
    )(window_start, z)


def solution(mesh):
    in_specs = (
        P(("parts", "genes"), "samples"),
        P(("parts", "genes"), "samples"),
        P(("parts", "samples", "genes"), None),
        P("parts", None),
        P("parts", None),
        P("parts"),
        P(("parts", "genes")),
    )
    out_specs = P(("parts", "genes"), None, "samples")
    return jax.shard_map(shards, mesh=mesh, in_specs=in_specs, out_specs=out_specs, check_vma=False)
```

```python
import functools

import jax
import jax.numpy as jnp
from jax import lax
from jax.experimental import pallas as pl
from jax.experimental.pallas import tpu as pltpu
from jax.sharding import PartitionSpec as P

W = 2048
HALF = 1024
SLOTS = 40
ALIGN = 128
PHEN = 41
ROWS = 336
USED = 328
RATIOS = 320
STEP = 256
GENE_DEV = 8
LANES = 384
SIDE = 8
MESH = pl.DeviceIdType.MESH
NT = (((1,), (1,)), ((), ()))


def mod(value, size):
    return value & (size - 1) if size & (size - 1) == 0 else lax.rem(value, size)


def permuted(counts_ref, block_ref, msgs_ref, owner):
    lane = lax.broadcasted_iota(jnp.int32, (16, ALIGN), 1)
    tiles = [jnp.zeros((16, ALIGN), jnp.float32) for _ in range(3)]
    for j in range(GENE_DEV):
        tile = block_ref[0, owner * GENE_DEV + j]
        start = block_ref[1, owner * GENE_DEV + j]
        a = counts_ref[tile].astype(jnp.float32)
        b = counts_ref[tile + 1].astype(jnp.float32)
        q = j * SLOTS % ALIGN
        turn = q - jnp.broadcast_to(start, (16, ALIGN))
        gene = jnp.where(lane >= start, a, b)
        for bit in (8, 16, 32, 64):
            gene = jnp.where((turn & bit) != 0, pltpu.roll(gene, bit, 1), gene)
        t = j * SLOTS // ALIGN
        tiles[t] = jnp.where((lane >= q) & (lane < q + SLOTS), gene, tiles[t])
        if q + SLOTS > ALIGN:
            tiles[t + 1] = jnp.where(lane < q + SLOTS - ALIGN, gene, tiles[t + 1])
    msgs_ref[owner] = jnp.concatenate(tiles, axis=1).astype(jnp.bfloat16)


def membership(sizes_ref, mask_ref, owner, sd_ref):
    per = ALIGN // GENE_DEV
    at = pl.ds(pl.multiple_of(owner // per * ALIGN, ALIGN), ALIGN)
    turn = (ALIGN - owner % per * GENE_DEV) % ALIGN
    sizes = pltpu.roll(sizes_ref[:, at].astype(jnp.float32), turn, 1)
    mask = pltpu.roll(mask_ref[:, at].astype(jnp.float32), turn, 1)
    slot = lax.broadcasted_iota(jnp.int32, (SLOTS, ALIGN), 0).astype(jnp.float32)
    ends = jnp.zeros((1, ALIGN), jnp.float32)
    cluster = jnp.zeros((SLOTS, ALIGN), jnp.float32)
    for c in range(8):
        ends = ends + sizes[c : c + 1]
        cluster = cluster + (ends <= slot).astype(jnp.float32)

    gene = lax.broadcasted_iota(jnp.int32, (SLOTS, GENE_DEV, ALIGN), 1)
    lane = lax.broadcasted_iota(jnp.int32, (SLOTS, GENE_DEV, ALIGN), 2)
    key = jnp.where(lane == gene, cluster[:, None, :], 0.0)
    key = jnp.sum(key, axis=2, keepdims=True).reshape(RATIOS, 1)
    row = lax.broadcasted_iota(jnp.int32, (RATIOS, 1), 0)
    row_gene = row & (GENE_DEV - 1)
    row_slot = lax.shift_right_logical(row, 3)
    row_key = key + (row_gene * 16).astype(jnp.float32)
    row_spot = row_gene * SLOTS + row_slot

    spot = lax.broadcasted_iota(jnp.int32, (ALIGN, LANES), 1)
    spot_gene = sum((spot >= SLOTS * g).astype(jnp.int32) for g in range(1, GENE_DEV + 1))
    pick = (lax.broadcasted_iota(jnp.int32, (ALIGN, LANES), 0) == spot_gene).astype(jnp.float32)
    spot, spot_gene = spot[:SLOTS], spot_gene[:SLOTS]
    here = lax.broadcasted_iota(jnp.int32, (SLOTS, LANES), 0) == spot - spot_gene * SLOTS

    def laid(value):
        full = lax.dot_general(
            value,
            pick,
            (((1,), (0,)), ((), ())),
            precision=lax.Precision.HIGHEST,
            preferred_element_type=jnp.float32,
        )
        return jnp.sum(jnp.where(here, full, 0.0), axis=0, keepdims=True)

    live = (laid(mask) > 0.5) & (spot[:1] < RATIOS)
    lane_key = jnp.where(live, laid(cluster) + (spot_gene[:1] * 16).astype(jnp.float32), -1.0)
    lane_spot = jnp.where(live, spot[:1], -1)
    sd_ref[:RATIOS] = (row_key == lane_key).astype(jnp.float32).astype(jnp.bfloat16)
    sd_ref[RATIOS:] = (row_spot == lane_spot).astype(jnp.float32).astype(jnp.bfloat16)


def kernel(
    n,
    block_ref,
    counts_hbm,
    expr_ref,
    sizes_ref,
    mask_ref,
    dose_ref,
    z_ref,
    counts_flat,
    counts_ref,
    msgs,
    raw,
    expr,
    panel,
    dose,
    squares,
    stat,
    pstat,
    sd,
    back,
    direct_sem,
    relay_sem,
    panel_sem,
    sent_sem,
    local_sem,
    dose_sem,
    expr_sem,
    back_sem,
    counts_sem,
):
    me = lax.axis_index("genes")
    core = lax.axis_index("samples")
    x, y = lax.shift_right_logical(me, 3), me & (SIDE - 1)
    nxt, prv = mod(me + 1, n), mod(me + n - 1, n)
    other = 1 - core
    xp = jnp.where(y > 0, x, mod(x + SIDE - 1, SIDE))

    load = pltpu.make_async_copy(counts_hbm, counts_flat, counts_sem)
    load.start()
    barrier = pltpu.get_barrier_semaphore()
    pl.semaphore_signal(barrier, inc=1, device_id={"samples": other}, device_id_type=MESH)

    @pl.loop(1, n)
    def _(step):
        pl.semaphore_signal(
            barrier, inc=1, device_id={"genes": mod(me + step, n)}, device_id_type=MESH
        )

    mine = pltpu.make_async_copy(dose_ref, dose.at[0], local_sem)
    mine.start()

    def chunk(i):
        half = lax.shift_right_logical(i + 1, 1)
        return jnp.where((i & 1) == 1, half, mod(SIDE - half, SIDE))

    def send_chunk(dx):
        @pl.loop(0, SIDE)
        def _(yo):
            owner = mod(x + dx, SIDE) * SIDE + yo
            near = mod(yo - y + SIDE, SIDE) < SIDE // 2
            kind = jnp.where(near, 0, 1)
            dest = jnp.where(near, owner, mod(owner + 1, n))

            @pl.when(dest != me)
            def _():
                pltpu.make_async_remote_copy(
                    src_ref=msgs.at[owner],
                    dst_ref=raw.at[kind, me],
                    send_sem=sent_sem.at[0],
                    recv_sem=direct_sem.at[kind, dx],
                    device_id={"genes": dest},
                    device_id_type=MESH,
                ).start()

            @pl.when(dest == me)
            def _():
                pltpu.make_async_copy(
                    msgs.at[owner], raw.at[kind, me], direct_sem.at[kind, dx]
                ).start()

    load.wait()
    with jax.named_scope("permute"):
        for t in range(counts_flat.shape[1] // ALIGN):
            counts_ref[t] = counts_flat[:, t * ALIGN : (t + 1) * ALIGN]
        counts_ref[counts_ref.shape[0] - 1] = counts_flat[:, :ALIGN]

        @pl.loop(0, n)
        def _(owner):
            permuted(counts_ref, block_ref, msgs, owner)

    with jax.named_scope("keys"):
        for kind, owner in enumerate((me, prv)):
            membership(sizes_ref, mask_ref, owner, sd.at[kind])
    expr[0] = expr_ref[...]
    with jax.named_scope("barrier"):
        pl.semaphore_wait(barrier, n)
    expr_copy = pltpu.make_async_remote_copy(
        src_ref=expr_ref,
        dst_ref=expr.at[1],
        send_sem=expr_sem.at[0],
        recv_sem=expr_sem.at[1],
        device_id={"genes": nxt},
        device_id_type=MESH,
    )
    expr_copy.start()
    with jax.named_scope("send"):

        @pl.loop(0, SIDE)
        def _(i):
            send_chunk(chunk(i))

    dose_copy = pltpu.make_async_remote_copy(
        src_ref=dose_ref,
        dst_ref=dose.at[1],
        send_sem=dose_sem.at[0],
        recv_sem=dose_sem.at[1],
        device_id={"samples": other},
        device_id_type=MESH,
    )
    dose_copy.start()
    mine.wait()

    def dose_squares(slot, first, rows):
        for r in range(rows // ALIGN):
            at = pl.ds(pl.multiple_of(first + r * ALIGN, ALIGN), ALIGN)
            square = jnp.zeros((ALIGN, ALIGN), jnp.float32) if slot == 0 else squares[at]
            for k in range(HALF // ALIGN):
                value = dose[slot, at, k * ALIGN : (k + 1) * ALIGN].astype(jnp.float32)
                square = square + value * value
            squares[at] = square

    def relay_chunk(dx):
        for kind in range(2):
            pltpu.make_async_copy(
                raw.at[kind, 0 : SIDE // 2], raw.at[kind, 0 : SIDE // 2], direct_sem.at[kind, dx]
            ).wait()
        for kind, partner in ((0, nxt), (1, prv)):
            xs = mod((x if kind == 0 else xp) + SIDE - dx, SIDE)

            @pl.loop(0, SIDE // 2)
            def _(t):
                ys = mod(y + SIDE - t, SIDE) if kind == 0 else mod(y + t, SIDE)
                source = xs * SIDE + ys
                pltpu.make_async_remote_copy(
                    src_ref=raw.at[kind, source],
                    dst_ref=raw.at[1 - kind, source],
                    send_sem=sent_sem.at[1],
                    recv_sem=relay_sem.at[1 - kind, dx],
                    device_id={"genes": partner},
                    device_id_type=MESH,
                ).start()

    def ratio_chunk(dx):
        for kind in range(2):
            pltpu.make_async_copy(
                raw.at[kind, 0 : SIDE // 2], raw.at[kind, 0 : SIDE // 2], relay_sem.at[kind, dx]
            ).wait()
            xs = mod((x if kind == 0 else xp) + SIDE - dx, SIDE)
            counts = raw[kind, pl.ds(xs * SIDE, SIDE)].reshape(ALIGN, LANES)
            both = lax.dot_general(sd[kind], counts, NT, preferred_element_type=jnp.float32)
            ratio = both[RATIOS:] / jnp.maximum(both[:RATIOS], 1.0)
            own = expr[kind, :, pl.ds(pl.multiple_of(xs * ALIGN, ALIGN), ALIGN)].astype(jnp.float32)
            rest = jnp.ones((ROWS - USED, ALIGN), jnp.float32)
            panel[kind, 0, xs] = jnp.concatenate([own, ratio, rest], axis=0).astype(jnp.bfloat16)

    def panel_copy(kind, dx):
        xs = mod((x if kind == 0 else xp) + SIDE - dx, SIDE)
        return pltpu.make_async_remote_copy(
            src_ref=panel.at[kind, 0, xs],
            dst_ref=panel.at[kind, 1, xs],
            send_sem=panel_sem.at[kind, 0],
            recv_sem=panel_sem.at[kind, 1],
            device_id={"samples": other},
            device_id_type=MESH,
        )

    def panel_chunk(dx):
        panel_copy(0, dx).start()

        @pl.when(core == 0)
        def _():
            panel_copy(1, dx).start()

    def pass_on(i, slot):
        with jax.named_scope("squares"):
            dose_squares(slot, (i & (SIDE // 2 - 1)) * 512, 512)
        with jax.named_scope("relay"):
            relay_chunk(chunk(i))

    pass_on(0, 0)
    pass_on(1, 0)
    expr_copy.wait()

    @pl.loop(2, SIDE // 2)
    def _(i):
        pass_on(i, 0)
        with jax.named_scope("ratio"):
            ratio_chunk(chunk(i - 2))

    with jax.named_scope("dose_wait"):
        dose_copy.wait_recv()

    @pl.loop(SIDE // 2, SIDE)
    def _(i):
        pass_on(i, 1)
        with jax.named_scope("ratio"):
            ratio_chunk(chunk(i - 2))
        panel_chunk(chunk(i - 4))

    count = float(2 * HALF)
    with jax.named_scope("square_rows"):
        for c in range(W // 512):
            at = slice(c * 512, (c + 1) * 512)
            stat[:, at] = lax.dot_general(
                jnp.ones((8, ALIGN), jnp.float32),
                squares[at],
                NT,
                precision=lax.Precision.HIGHEST,
                preferred_element_type=jnp.float32,
            )

    panel_chunk(chunk(SIDE - 4))
    panel_chunk(chunk(SIDE - 3))
    with jax.named_scope("ratio_end"):
        ratio_chunk(chunk(SIDE - 2))
    with jax.named_scope("ratio_end"):
        ratio_chunk(chunk(SIDE - 1))
    panel_chunk(chunk(SIDE - 2))
    panel_chunk(chunk(SIDE - 1))

    def panel_wait(kind, way):
        pltpu.make_async_copy(panel.at[kind, 1], panel.at[kind, 1], panel_sem.at[kind, way]).wait()

    with jax.named_scope("panel_wait"):
        panel_wait(0, 1)

    @pl.when(core == 1)
    def _():
        panel_wait(1, 1)

    def pheno_stats(kind):
        PIECE = 48
        for g in range(ROWS // PIECE):
            rows = slice(g * PIECE, (g + 1) * PIECE)
            total = jnp.zeros((PIECE, ALIGN), jnp.float32)
            square = jnp.zeros((PIECE, ALIGN), jnp.float32)
            for slot in range(2):
                for k in range(SIDE):
                    value = panel[kind, slot, k, rows].astype(jnp.float32)
                    total = total + value
                    square = square + value * value
            total = jnp.sum(total, axis=1, keepdims=True)
            square = jnp.sum(square, axis=1, keepdims=True)
            pstat[0, rows] = jnp.broadcast_to(total, (PIECE, ALIGN))
            scale = lax.rsqrt(jnp.maximum(square - total * total / count, 1.0))
            pstat[1, rows] = jnp.broadcast_to(scale, (PIECE, ALIGN))

    def assoc(kind, first, out_ref, scale, after=None):
        left = [
            jnp.concatenate([panel[kind, slot, k] for k in range(SIDE)], axis=1) for slot in range(2)
        ]

        @pl.loop(0, HALF // STEP)
        def _(c):
            at = pl.multiple_of(first + c * STEP, STEP)
            product = sum(
                lax.dot_general(
                    left[slot], dose[slot, pl.ds(at, STEP)], NT, preferred_element_type=jnp.float32
                )
                for slot in range(2)
            )
            for k in range(STEP // ALIGN):
                here = pl.ds(pl.multiple_of(at + k * ALIGN, ALIGN), ALIGN)
                part = product[:, k * ALIGN : (k + 1) * ALIGN]
                total = part[USED : USED + 1]
                mean = total * (1.0 / count)
                dev = lax.rsqrt(jnp.maximum(stat[0:1, here] - total * mean, 1.0)) * scale
                part = (part - pstat[0] * mean) * dev * pstat[1]
                out_ref[c, :, k * ALIGN : (k + 1) * ALIGN] = part.astype(jnp.bfloat16)
            if after is not None:

                @pl.when(c > 0)
                def _():
                    after(c - 1)

        if after is not None:
            after(HALF // STEP - 1)

    keep = jnp.where(me == 0, 0.0, 1.0)

    def give(c):
        return pltpu.make_async_remote_copy(
            src_ref=back.at[c],
            dst_ref=z_ref.at[1, c],
            send_sem=back_sem.at[0],
            recv_sem=back_sem.at[1],
            device_id={"genes": prv},
            device_id_type=MESH,
        )

    @pl.when(core == 0)
    def _():
        with jax.named_scope("pstats_a"):
            pheno_stats(0)
        with jax.named_scope("assoc_a"):
            assoc(0, 0, z_ref.at[0], 1.0)
            assoc(0, HALF, z_ref.at[1], 1.0)

    @pl.when(core == 1)
    def _():
        with jax.named_scope("pstats_b"):
            pheno_stats(1)
        with jax.named_scope("assoc_b"):
            assoc(1, 0, back, keep, lambda c: give(c).start())
        with jax.named_scope("assoc_c"):
            pheno_stats(0)
            assoc(0, HALF, z_ref.at[0], 1.0)
        with jax.named_scope("back_wait"):
            for way in (1, 0):
                pltpu.make_async_copy(back, back, back_sem.at[way]).wait()

    dose_copy.wait_send()
    pltpu.make_async_copy(raw.at[0, 0 : n - 2], raw.at[0, 0 : n - 2], sent_sem.at[0]).wait()
    pltpu.make_async_copy(raw.at[0], raw.at[0], sent_sem.at[1]).wait()
    panel_wait(0, 0)

    @pl.when(core == 0)
    def _():
        panel_wait(1, 0)


def cut(start_ref, z_ref, out_ref):
    gene = lax.broadcasted_iota(jnp.int32, (ROWS, ALIGN), 0) & (GENE_DEV - 1)

    @pl.loop(0, HALF // ALIGN)
    def _(m):
        part = None
        for g in range(GENE_DEV):
            t = lax.shift_right_logical(start_ref[g], 7) + m
            half = lax.shift_right_logical(t, 3)
            step = lax.shift_right_logical(t, 1) & (HALF // STEP - 1)
            lanes = pl.ds(pl.multiple_of((t & 1) * ALIGN, ALIGN), ALIGN)
            value = z_ref[half, step, :, lanes]
            part = value if g == 0 else jnp.where(gene == g, value, part)
        to = pl.ds(pl.multiple_of(m * ALIGN, ALIGN), ALIGN)
        out_ref[:, :, to] = part[:USED].reshape(PHEN, GENE_DEV, ALIGN)


def shards(dosage, expression, intron_counts, cluster_sizes, valid_mask, gene_block, window_start):
    n = lax.axis_size("genes")
    vmem = pl.BlockSpec(memory_space=pltpu.VMEM)
    smem = pl.BlockSpec(memory_space=pltpu.SMEM)
    hbm = pl.BlockSpec(memory_space=pl.ANY)
    dma = pltpu.SemaphoreType.DMA
    bf16, f32 = jnp.bfloat16, jnp.float32
    z = pl.pallas_call(
        functools.partial(kernel, n),
        out_shape=jax.ShapeDtypeStruct((2, HALF // STEP, ROWS, STEP), bf16),
        in_specs=[smem, hbm, vmem, vmem, vmem, hbm],
        out_specs=vmem,
        scratch_shapes=[
            pltpu.VMEM(intron_counts.shape, bf16),
            pltpu.VMEM((intron_counts.shape[1] // ALIGN + 1, 16, ALIGN), bf16),
            pltpu.VMEM((n, 16, LANES), bf16),
            pltpu.VMEM((2, n, 16, LANES), bf16),
            pltpu.VMEM((2, GENE_DEV, HALF), bf16),
            pltpu.VMEM((2, 2, SIDE, ROWS, ALIGN), bf16),
            pltpu.VMEM((2, W, HALF), bf16),
            pltpu.VMEM((W, ALIGN), f32),
            pltpu.VMEM((8, W), f32),
            pltpu.VMEM((2, ROWS, ALIGN), f32),
            pltpu.VMEM((2, 2 * RATIOS, LANES), bf16),
            pltpu.VMEM((HALF // STEP, ROWS, STEP), bf16),
            dma((2, SIDE)),
            dma((2, SIDE)),
            dma((2, 2)),
            dma((2,)),
            dma,
            dma((2,)),
            dma((2,)),
            dma((2,)),
            dma,
        ],
        compiler_params=pltpu.CompilerParams(collective_id=0, has_side_effects=True),
        name="associate",
    )(
        jnp.stack([gene_block * SLOTS // ALIGN, gene_block * SLOTS % ALIGN]),
        intron_counts,
        expression,
        cluster_sizes.T,
        valid_mask.T,
        dosage,
    )
    out = pl.pallas_call(
        cut,
        out_shape=jax.ShapeDtypeStruct((PHEN, GENE_DEV, HALF), bf16),
        in_specs=[smem, vmem],
        out_specs=vmem,
        name="cut",
    )(window_start, z)
    return jnp.swapaxes(out, 0, 1)


def solution(mesh):
    in_specs = (
        P(("parts", "genes"), "samples"),
        P(("parts", "genes"), "samples"),
        P(("parts", "samples", "genes"), None),
        P("parts", None),
        P("parts", None),
        P("parts"),
        P(("parts", "genes")),
    )
    out_specs = P(("parts", "genes"), None, "samples")
    return jax.shard_map(shards, mesh=mesh, in_specs=in_specs, out_specs=out_specs, check_vma=False)
```

```python
import functools

import jax
import jax.numpy as jnp
from jax import lax
from jax.experimental import pallas as pl
from jax.experimental.pallas import tpu as pltpu
from jax.sharding import PartitionSpec as P

W = 2048
HALF = 1024
SLOTS = 40
ALIGN = 128
PHEN = 41
ROWS = 336
USED = 328
RATIOS = 320
STEP = 256
GENE_DEV = 8
LANES = 384
SIDE = 8
MESH = pl.DeviceIdType.MESH
NT = (((1,), (1,)), ((), ()))


def mod(value, size):
    return value & (size - 1) if size & (size - 1) == 0 else lax.rem(value, size)


def permuted(counts_ref, block_ref, msgs_ref, owner):
    lane = lax.broadcasted_iota(jnp.int32, (16, ALIGN), 1)
    tiles = [None] * 3
    for j in range(GENE_DEV):
        first = block_ref[owner * GENE_DEV + j] * SLOTS
        tile = lax.shift_right_logical(first, 7)
        start = first & (ALIGN - 1)
        a = counts_ref[tile].astype(jnp.float32)
        b = counts_ref[tile + 1].astype(jnp.float32)
        q = j * SLOTS % ALIGN
        gene = pltpu.roll(jnp.where(lane >= start, a, b), (q - start) & (ALIGN - 1), 1)
        t = j * SLOTS // ALIGN
        tiles[t] = gene if q == 0 else jnp.where(lane >= q, gene, tiles[t])
        if q + SLOTS > ALIGN:
            tiles[t + 1] = gene
    packed = jnp.where(lane[:8] < ALIGN // 2, tiles[2][:8], pltpu.roll(tiles[2][8:], ALIGN // 2, 1))
    msgs_ref[owner] = jnp.concatenate([tiles[0], tiles[1], packed], axis=0).astype(jnp.bfloat16)


def membership(sizes_ref, mask_ref, owner, sd_ref):
    per = ALIGN // GENE_DEV
    at = pl.ds(pl.multiple_of(owner // per * ALIGN, ALIGN), ALIGN)
    turn = (ALIGN - owner % per * GENE_DEV) % ALIGN
    sizes = pltpu.roll(sizes_ref[:, at].astype(jnp.float32), turn, 1)
    mask = pltpu.roll(mask_ref[:, at].astype(jnp.float32), turn, 1)
    slot = lax.broadcasted_iota(jnp.int32, (SLOTS, ALIGN), 0).astype(jnp.float32)
    ends = jnp.zeros((1, ALIGN), jnp.float32)
    cluster = jnp.zeros((SLOTS, ALIGN), jnp.float32)
    for c in range(8):
        ends = ends + sizes[c : c + 1]
        cluster = cluster + (ends <= slot).astype(jnp.float32)

    gene = lax.broadcasted_iota(jnp.int32, (SLOTS, GENE_DEV, ALIGN), 1)
    lane = lax.broadcasted_iota(jnp.int32, (SLOTS, GENE_DEV, ALIGN), 2)
    key = jnp.where(lane == gene, cluster[:, None, :], 0.0)
    key = jnp.sum(key, axis=2, keepdims=True).reshape(RATIOS, 1)
    row = lax.broadcasted_iota(jnp.int32, (RATIOS, 1), 0)
    row_gene = row & (GENE_DEV - 1)
    row_slot = lax.shift_right_logical(row, 3)
    row_key = key + (row_gene * 16).astype(jnp.float32)
    row_spot = row_gene * SLOTS + row_slot

    spot = lax.broadcasted_iota(jnp.int32, (ALIGN, LANES), 1)
    spot_gene = sum((spot >= SLOTS * g).astype(jnp.int32) for g in range(1, GENE_DEV + 1))
    pick = (lax.broadcasted_iota(jnp.int32, (ALIGN, LANES), 0) == spot_gene).astype(jnp.float32)
    spot, spot_gene = spot[:SLOTS], spot_gene[:SLOTS]
    here = lax.broadcasted_iota(jnp.int32, (SLOTS, LANES), 0) == spot - spot_gene * SLOTS

    def laid(value):
        full = lax.dot_general(
            value,
            pick,
            (((1,), (0,)), ((), ())),
            precision=lax.Precision.HIGHEST,
            preferred_element_type=jnp.float32,
        )
        return jnp.sum(jnp.where(here, full, 0.0), axis=0, keepdims=True)

    live = (laid(mask) > 0.5) & (spot[:1] < RATIOS)
    lane_key = jnp.where(live, laid(cluster) + (spot_gene[:1] * 16).astype(jnp.float32), -1.0)
    lane_spot = jnp.where(live, spot[:1], -1)
    sd_ref[:RATIOS] = (row_key == lane_key).astype(jnp.float32).astype(jnp.bfloat16)
    sd_ref[RATIOS:] = (row_spot == lane_spot).astype(jnp.float32).astype(jnp.bfloat16)


def kernel(
    n,
    block_hbm,
    start_hbm,
    counts_hbm,
    expr_ref,
    sizes_hbm,
    mask_hbm,
    dose_ref,
    out_ref,
    block_ref,
    start_ref,
    sizes_ref,
    mask_ref,
    z_ref,
    counts_flat,
    counts_ref,
    msgs,
    raw,
    expr,
    panel,
    dose,
    squares,
    stat,
    pstat,
    sd,
    back,
    direct_sem,
    relay_sem,
    panel_sem,
    sent_sem,
    local_sem,
    dose_sem,
    expr_sem,
    back_sem,
    load_sem,
):
    me = lax.axis_index("genes")
    core = lax.axis_index("samples")
    x, y = lax.shift_right_logical(me, 3), me & (SIDE - 1)
    nxt, prv = mod(me + 1, n), mod(me + n - 1, n)
    other = 1 - core
    xp = jnp.where(y > 0, x, mod(x + SIDE - 1, SIDE))

    loads = [
        pltpu.make_async_copy(source, to, load_sem.at[k])
        for k, (source, to) in enumerate(
            (
                (counts_hbm, counts_flat),
                (block_hbm, block_ref),
                (start_hbm, start_ref),
                (sizes_hbm, sizes_ref),
                (mask_hbm, mask_ref),
                (expr_ref, expr.at[0]),
            )
        )
    ]
    for load in loads:
        load.start()
    barrier = pltpu.get_barrier_semaphore()
    pl.semaphore_signal(barrier, inc=1, device_id={"samples": other}, device_id_type=MESH)

    @pl.loop(1, n)
    def _(step):
        pl.semaphore_signal(
            barrier, inc=1, device_id={"genes": mod(me + step, n)}, device_id_type=MESH
        )

    mine = pltpu.make_async_copy(dose_ref, dose.at[0], local_sem)
    mine.start()

    def chunk(i):
        half = lax.shift_right_logical(i + 1, 1)
        return jnp.where((i & 1) == 1, half, mod(SIDE - half, SIDE))

    def send_chunk(dx):
        @pl.loop(0, SIDE)
        def _(yo):
            owner = mod(x + dx, SIDE) * SIDE + yo
            near = mod(yo - y + SIDE, SIDE) < SIDE // 2
            kind = jnp.where(near, 0, 1)
            dest = jnp.where(near, owner, mod(owner + 1, n))

            @pl.when(dest != me)
            def _():
                pltpu.make_async_remote_copy(
                    src_ref=msgs.at[owner],
                    dst_ref=raw.at[kind, me],
                    send_sem=sent_sem.at[0],
                    recv_sem=direct_sem.at[kind, dx],
                    device_id={"genes": dest},
                    device_id_type=MESH,
                ).start()

            @pl.when(dest == me)
            def _():
                pltpu.make_async_copy(
                    msgs.at[owner], raw.at[kind, me], direct_sem.at[kind, dx]
                ).start()

    for load in loads:
        load.wait()
    with jax.named_scope("permute"):
        for t in range(counts_flat.shape[1] // ALIGN):
            counts_ref[t] = counts_flat[:, t * ALIGN : (t + 1) * ALIGN]
        counts_ref[counts_ref.shape[0] - 1] = counts_flat[:, :ALIGN]

        @pl.loop(0, n, unroll=8)
        def _(owner):
            permuted(counts_ref, block_ref, msgs, owner)

    with jax.named_scope("keys"):
        for kind, owner in enumerate((me, prv)):
            membership(sizes_ref, mask_ref, owner, sd.at[kind])
    with jax.named_scope("barrier"):
        pl.semaphore_wait(barrier, n)
    expr_copy = pltpu.make_async_remote_copy(
        src_ref=expr_ref,
        dst_ref=expr.at[1],
        send_sem=expr_sem.at[0],
        recv_sem=expr_sem.at[1],
        device_id={"genes": nxt},
        device_id_type=MESH,
    )
    expr_copy.start()
    with jax.named_scope("send"):

        @pl.loop(0, SIDE)
        def _(i):
            send_chunk(chunk(i))

    dose_copy = pltpu.make_async_remote_copy(
        src_ref=dose_ref,
        dst_ref=dose.at[1],
        send_sem=dose_sem.at[0],
        recv_sem=dose_sem.at[1],
        device_id={"samples": other},
        device_id_type=MESH,
    )
    dose_copy.start()
    mine.wait()

    def dose_squares(slot, first, rows):
        for r in range(rows // ALIGN):
            at = pl.ds(pl.multiple_of(first + r * ALIGN, ALIGN), ALIGN)
            square = jnp.zeros((ALIGN, ALIGN), jnp.float32) if slot == 0 else squares[at]
            for k in range(HALF // ALIGN):
                value = dose[slot, at, k * ALIGN : (k + 1) * ALIGN].astype(jnp.float32)
                square = square + value * value
            squares[at] = square

    def relay_chunk(dx):
        for kind in range(2):
            pltpu.make_async_copy(
                raw.at[kind, 0 : SIDE // 2], raw.at[kind, 0 : SIDE // 2], direct_sem.at[kind, dx]
            ).wait()
        for kind, partner in ((0, nxt), (1, prv)):
            xs = mod((x if kind == 0 else xp) + SIDE - dx, SIDE)

            @pl.loop(0, SIDE // 2)
            def _(t):
                ys = mod(y + SIDE - t, SIDE) if kind == 0 else mod(y + t, SIDE)
                source = xs * SIDE + ys
                pltpu.make_async_remote_copy(
                    src_ref=raw.at[kind, source],
                    dst_ref=raw.at[1 - kind, source],
                    send_sem=sent_sem.at[1],
                    recv_sem=relay_sem.at[1 - kind, dx],
                    device_id={"genes": partner},
                    device_id_type=MESH,
                ).start()

    def ratio_chunk(dx):
        for kind in range(2):
            pltpu.make_async_copy(
                raw.at[kind, 0 : SIDE // 2], raw.at[kind, 0 : SIDE // 2], relay_sem.at[kind, dx]
            ).wait()
            xs = mod((x if kind == 0 else xp) + SIDE - dx, SIDE)
            at = pl.ds(xs * SIDE, SIDE)
            low = raw[kind, at, :16].reshape(ALIGN, ALIGN)
            high = raw[kind, at, 16:32].reshape(ALIGN, ALIGN)
            left = raw[kind, at, 32:].astype(jnp.float32)
            right = pltpu.roll(left, ALIGN // 2, 2)
            last = jnp.concatenate([left, right], axis=1).reshape(ALIGN, ALIGN).astype(jnp.bfloat16)
            counts = jnp.concatenate([low, high, last], axis=1)
            both = lax.dot_general(sd[kind], counts, NT, preferred_element_type=jnp.float32)
            ratio = both[RATIOS:] / jnp.maximum(both[:RATIOS], 1.0)
            own = expr[kind, :, pl.ds(pl.multiple_of(xs * ALIGN, ALIGN), ALIGN)].astype(jnp.float32)
            rest = jnp.ones((ROWS - USED, ALIGN), jnp.float32)
            panel[kind, 0, xs] = jnp.concatenate([own, ratio, rest], axis=0).astype(jnp.bfloat16)

    def panel_copy(kind, dx):
        xs = mod((x if kind == 0 else xp) + SIDE - dx, SIDE)
        return pltpu.make_async_remote_copy(
            src_ref=panel.at[kind, 0, xs],
            dst_ref=panel.at[kind, 1, xs],
            send_sem=panel_sem.at[kind, 0],
            recv_sem=panel_sem.at[kind, 1],
            device_id={"samples": other},
            device_id_type=MESH,
        )

    def panel_chunk(dx):
        panel_copy(0, dx).start()

        @pl.when(core == 0)
        def _():
            panel_copy(1, dx).start()

    def pass_on(i, slot=None):
        if slot is not None:
            with jax.named_scope("squares"):
                dose_squares(slot, i * 512, 512)
        with jax.named_scope("relay"):
            relay_chunk(chunk(i))

    pass_on(0, 0)
    pass_on(1, 0)
    expr_copy.wait()

    @pl.loop(2, SIDE // 2)
    def _(i):
        pass_on(i, 0)
        with jax.named_scope("ratio"):
            ratio_chunk(chunk(i - 2))

    @pl.loop(SIDE // 2, SIDE)
    def _(i):
        pass_on(i)
        with jax.named_scope("ratio"):
            ratio_chunk(chunk(i - 2))
        panel_chunk(chunk(i - 4))

    with jax.named_scope("dose_wait"):
        dose_copy.wait_recv()
    with jax.named_scope("squares_1"):

        @pl.loop(0, W // 512)
        def _(i):
            dose_squares(1, i * 512, 512)

    count = float(2 * HALF)
    with jax.named_scope("square_rows"):
        for c in range(W // 512):
            at = slice(c * 512, (c + 1) * 512)
            stat[:, at] = lax.dot_general(
                jnp.ones((8, ALIGN), jnp.float32),
                squares[at],
                NT,
                precision=lax.Precision.HIGHEST,
                preferred_element_type=jnp.float32,
            )

    panel_chunk(chunk(SIDE - 4))
    panel_chunk(chunk(SIDE - 3))
    with jax.named_scope("ratio_end"):
        ratio_chunk(chunk(SIDE - 2))
    with jax.named_scope("ratio_end"):
        ratio_chunk(chunk(SIDE - 1))
    panel_chunk(chunk(SIDE - 2))
    panel_chunk(chunk(SIDE - 1))

    def panel_wait(kind, way):
        pltpu.make_async_copy(panel.at[kind, 1], panel.at[kind, 1], panel_sem.at[kind, way]).wait()

    with jax.named_scope("panel_wait"):
        panel_wait(0, 1)

    @pl.when(core == 1)
    def _():
        panel_wait(1, 1)

    def pheno_stats(kind):
        PIECE = 48
        for g in range(ROWS // PIECE):
            rows = slice(g * PIECE, (g + 1) * PIECE)
            total = jnp.zeros((PIECE, ALIGN), jnp.float32)
            square = jnp.zeros((PIECE, ALIGN), jnp.float32)
            for slot in range(2):
                for k in range(SIDE):
                    value = panel[kind, slot, k, rows].astype(jnp.float32)
                    total = total + value
                    square = square + value * value
            total = jnp.sum(total, axis=1, keepdims=True)
            square = jnp.sum(square, axis=1, keepdims=True)
            pstat[0, rows] = jnp.broadcast_to(total, (PIECE, ALIGN))
            scale = lax.rsqrt(jnp.maximum(square - total * total / count, 1.0))
            pstat[1, rows] = jnp.broadcast_to(scale, (PIECE, ALIGN))

    def assoc(kind, first, to_ref, scale, after=None):
        left = [
            jnp.concatenate([panel[kind, slot, k] for k in range(SIDE)], axis=1) for slot in range(2)
        ]

        @pl.loop(0, HALF // STEP)
        def _(c):
            at = pl.multiple_of(first + c * STEP, STEP)
            product = sum(
                lax.dot_general(
                    left[slot], dose[slot, pl.ds(at, STEP)], NT, preferred_element_type=jnp.float32
                )
                for slot in range(2)
            )
            for k in range(STEP // ALIGN):
                here = pl.ds(pl.multiple_of(at + k * ALIGN, ALIGN), ALIGN)
                part = product[:, k * ALIGN : (k + 1) * ALIGN]
                total = part[USED : USED + 1]
                mean = total * (1.0 / count)
                dev = lax.rsqrt(jnp.maximum(stat[0:1, here] - total * mean, 1.0)) * scale
                part = (part - pstat[0] * mean) * dev * pstat[1]
                to_ref[c * (STEP // ALIGN) + k] = part.astype(jnp.bfloat16)
            if after is not None:

                @pl.when(c > 0)
                def _():
                    after(c - 1)

        if after is not None:
            after(HALF // STEP - 1)

    keep = jnp.where(me == 0, 0.0, 1.0)

    per = STEP // ALIGN
    first_half, second_half = z_ref.at[0:SIDE], z_ref.at[SIDE : 2 * SIDE]

    def give(c):
        return pltpu.make_async_remote_copy(
            src_ref=back.at[pl.ds(c * per, per)],
            dst_ref=z_ref.at[pl.ds(SIDE + c * per, per)],
            send_sem=back_sem.at[0],
            recv_sem=back_sem.at[1],
            device_id={"genes": prv},
            device_id_type=MESH,
        )

    @pl.when(core == 0)
    def _():
        with jax.named_scope("pstats_a"):
            pheno_stats(0)
        with jax.named_scope("assoc_a"):
            assoc(0, 0, first_half, 1.0)
            assoc(0, HALF, second_half, 1.0)

    @pl.when(core == 1)
    def _():
        with jax.named_scope("pstats_b"):
            pheno_stats(1)
        with jax.named_scope("assoc_b"):
            assoc(1, 0, back, keep, lambda c: give(c).start())
        with jax.named_scope("assoc_c"):
            pheno_stats(0)
            assoc(0, HALF, first_half, 1.0)
        with jax.named_scope("back_wait"):
            for way in (1, 0):
                pltpu.make_async_copy(back, back, back_sem.at[way]).wait()

    with jax.named_scope("cut"):
        gene = lax.broadcasted_iota(jnp.int32, (ROWS, ALIGN), 0) & (GENE_DEV - 1)

        @pl.loop(0, HALF // ALIGN)
        def _(m):
            part = None
            for g in range(GENE_DEV):
                value = z_ref[lax.shift_right_logical(start_ref[g], 7) + m]
                part = value if g == 0 else jnp.where(gene == g, value, part)
            to = pl.ds(pl.multiple_of(m * ALIGN, ALIGN), ALIGN)
            out_ref[:, :, to] = part[:USED].reshape(PHEN, GENE_DEV, ALIGN)

    dose_copy.wait_send()
    pltpu.make_async_copy(raw.at[0, 0 : n - 2], raw.at[0, 0 : n - 2], sent_sem.at[0]).wait()
    pltpu.make_async_copy(raw.at[0], raw.at[0], sent_sem.at[1]).wait()
    panel_wait(0, 0)

    @pl.when(core == 0)
    def _():
        panel_wait(1, 0)


def shards(dosage, expression, intron_counts, cluster_sizes, valid_mask, gene_block, window_start):
    n = lax.axis_size("genes")
    dma = pltpu.SemaphoreType.DMA
    bf16, f32 = jnp.bfloat16, jnp.float32
    out = pl.pallas_call(
        functools.partial(kernel, n),
        out_shape=jax.ShapeDtypeStruct((PHEN, GENE_DEV, HALF), bf16),
        in_specs=[pl.BlockSpec(memory_space=pl.ANY)] * 7,
        out_specs=pl.BlockSpec(memory_space=pltpu.VMEM),
        scratch_shapes=[
            pltpu.SMEM(gene_block.shape, jnp.int32),
            pltpu.SMEM(window_start.shape, jnp.int32),
            pltpu.VMEM(cluster_sizes.shape[::-1], jnp.int32),
            pltpu.VMEM(valid_mask.shape[::-1], jnp.int32),
            pltpu.VMEM((2 * SIDE, ROWS, ALIGN), bf16),
            pltpu.VMEM(intron_counts.shape, bf16),
            pltpu.VMEM((intron_counts.shape[1] // ALIGN + 1, 16, ALIGN), bf16),
            pltpu.VMEM((n, SLOTS, ALIGN), bf16),
            pltpu.VMEM((2, n, SLOTS, ALIGN), bf16),
            pltpu.VMEM((2, GENE_DEV, HALF), bf16),
            pltpu.VMEM((2, 2, SIDE, ROWS, ALIGN), bf16),
            pltpu.VMEM((2, W, HALF), bf16),
            pltpu.VMEM((W, ALIGN), f32),
            pltpu.VMEM((8, W), f32),
            pltpu.VMEM((2, ROWS, ALIGN), f32),
            pltpu.VMEM((2, 2 * RATIOS, LANES), bf16),
            pltpu.VMEM((SIDE, ROWS, ALIGN), bf16),
            dma((2, SIDE)),
            dma((2, SIDE)),
            dma((2, 2)),
            dma((2,)),
            dma,
            dma((2,)),
            dma((2,)),
            dma((2,)),
            dma((6,)),
        ],
        compiler_params=pltpu.CompilerParams(collective_id=0, has_side_effects=True),
        name="associate",
    )(
        gene_block,
        window_start,
        intron_counts,
        expression,
        cluster_sizes.T,
        valid_mask.T,
        dosage,
    )
    return jnp.swapaxes(out, 0, 1)


def solution(mesh):
    in_specs = (
        P(("parts", "genes"), "samples"),
        P(("parts", "genes"), "samples"),
        P(("parts", "samples", "genes"), None),
        P("parts", None),
        P("parts", None),
        P("parts"),
        P(("parts", "genes")),
    )
    out_specs = P(("parts", "genes"), None, "samples")
    return jax.shard_map(shards, mesh=mesh, in_specs=in_specs, out_specs=out_specs, check_vma=False)
```

```python
import functools

import jax
import jax.numpy as jnp
from jax import lax
from jax.experimental import pallas as pl
from jax.experimental.pallas import tpu as pltpu
from jax.sharding import PartitionSpec as P

W = 2048
HALF = 1024
SLOTS = 40
ALIGN = 128
PHEN = 41
ROWS = 336
USED = 328
RATIOS = 320
STEP = 256
GENE_DEV = 8
LANES = 384
SIDE = 8
MESH = pl.DeviceIdType.MESH
NT = (((1,), (1,)), ((), ()))


def mod(value, size):
    return value & (size - 1) if size & (size - 1) == 0 else lax.rem(value, size)


def permuted(counts_ref, block_ref, msgs_ref, owner):
    lane = lax.broadcasted_iota(jnp.int32, (16, ALIGN), 1)
    tiles = [None] * 3
    for j in range(GENE_DEV):
        first = block_ref[owner * GENE_DEV + j] * SLOTS
        tile = lax.shift_right_logical(first, 7)
        start = first & (ALIGN - 1)
        a = counts_ref[tile].astype(jnp.float32)
        b = counts_ref[tile + 1].astype(jnp.float32)
        q = j * SLOTS % ALIGN
        gene = pltpu.roll(jnp.where(lane >= start, a, b), (q - start) & (ALIGN - 1), 1)
        t = j * SLOTS // ALIGN
        tiles[t] = gene if q == 0 else jnp.where(lane >= q, gene, tiles[t])
        if q + SLOTS > ALIGN:
            tiles[t + 1] = gene
    packed = jnp.where(lane[:8] < ALIGN // 2, tiles[2][:8], pltpu.roll(tiles[2][8:], ALIGN // 2, 1))
    msgs_ref[owner] = jnp.concatenate([tiles[0], tiles[1], packed], axis=0).astype(jnp.bfloat16)


def membership(sizes_ref, mask_ref, owner, sd_ref):
    per = ALIGN // GENE_DEV
    at = pl.ds(pl.multiple_of(owner // per * ALIGN, ALIGN), ALIGN)
    turn = (ALIGN - owner % per * GENE_DEV) % ALIGN
    sizes = pltpu.roll(sizes_ref[:, at].astype(jnp.float32), turn, 1)
    mask = pltpu.roll(mask_ref[:, at].astype(jnp.float32), turn, 1)
    slot = lax.broadcasted_iota(jnp.int32, (SLOTS, ALIGN), 0).astype(jnp.float32)
    ends = jnp.zeros((1, ALIGN), jnp.float32)
    cluster = jnp.zeros((SLOTS, ALIGN), jnp.float32)
    for c in range(8):
        ends = ends + sizes[c : c + 1]
        cluster = cluster + (ends <= slot).astype(jnp.float32)

    gene = lax.broadcasted_iota(jnp.int32, (SLOTS, GENE_DEV, ALIGN), 1)
    lane = lax.broadcasted_iota(jnp.int32, (SLOTS, GENE_DEV, ALIGN), 2)
    key = jnp.where(lane == gene, cluster[:, None, :], 0.0)
    key = jnp.sum(key, axis=2, keepdims=True).reshape(RATIOS, 1)
    row = lax.broadcasted_iota(jnp.int32, (RATIOS, 1), 0)
    row_gene = row & (GENE_DEV - 1)
    row_slot = lax.shift_right_logical(row, 3)
    row_key = key + (row_gene * 16).astype(jnp.float32)
    row_spot = row_gene * SLOTS + row_slot

    spot = lax.broadcasted_iota(jnp.int32, (ALIGN, LANES), 1)
    spot_gene = sum((spot >= SLOTS * g).astype(jnp.int32) for g in range(1, GENE_DEV + 1))
    pick = (lax.broadcasted_iota(jnp.int32, (ALIGN, LANES), 0) == spot_gene).astype(jnp.float32)
    spot, spot_gene = spot[:SLOTS], spot_gene[:SLOTS]
    here = lax.broadcasted_iota(jnp.int32, (SLOTS, LANES), 0) == spot - spot_gene * SLOTS

    def laid(value):
        full = lax.dot_general(
            value,
            pick,
            (((1,), (0,)), ((), ())),
            precision=lax.Precision.HIGHEST,
            preferred_element_type=jnp.float32,
        )
        return jnp.sum(jnp.where(here, full, 0.0), axis=0, keepdims=True)

    live = (laid(mask) > 0.5) & (spot[:1] < RATIOS)
    lane_key = jnp.where(live, laid(cluster) + (spot_gene[:1] * 16).astype(jnp.float32), -1.0)
    lane_spot = jnp.where(live, spot[:1], -1)
    sd_ref[:RATIOS] = (row_key == lane_key).astype(jnp.float32).astype(jnp.bfloat16)
    sd_ref[RATIOS:] = (row_spot == lane_spot).astype(jnp.float32).astype(jnp.bfloat16)


def kernel(
    n,
    block_hbm,
    start_hbm,
    counts_hbm,
    expr_ref,
    sizes_hbm,
    mask_hbm,
    dose_ref,
    out_ref,
    block_ref,
    start_ref,
    sizes_ref,
    mask_ref,
    z_ref,
    counts_flat,
    counts_ref,
    msgs,
    raw,
    expr,
    panel,
    dose,
    squares,
    stat,
    pstat,
    sd,
    back,
    land,
    partial,
    result,
    direct_sem,
    relay_sem,
    panel_sem,
    sent_sem,
    local_sem,
    dose_sem,
    expr_sem,
    back_sem,
    back_send_sem,
    out_sem,
    load_sem,
):
    me = lax.axis_index("genes")
    core = lax.axis_index("samples")
    x, y = lax.shift_right_logical(me, 3), me & (SIDE - 1)
    nxt, prv = mod(me + 1, n), mod(me + n - 1, n)
    other = 1 - core
    xp = jnp.where(y > 0, x, mod(x + SIDE - 1, SIDE))

    loads = [
        pltpu.make_async_copy(source, to, load_sem.at[k])
        for k, (source, to) in enumerate(
            (
                (counts_hbm, counts_flat),
                (block_hbm, block_ref),
                (start_hbm, start_ref),
                (sizes_hbm, sizes_ref),
                (mask_hbm, mask_ref),
                (expr_ref, expr.at[0]),
            )
        )
    ]
    for load in loads:
        load.start()
    barrier = pltpu.get_barrier_semaphore()
    pl.semaphore_signal(barrier, inc=1, device_id={"samples": other}, device_id_type=MESH)

    @pl.loop(1, n)
    def _(step):
        pl.semaphore_signal(
            barrier, inc=1, device_id={"genes": mod(me + step, n)}, device_id_type=MESH
        )

    mine = pltpu.make_async_copy(dose_ref, dose.at[0], local_sem)
    mine.start()

    def chunk(i):
        half = lax.shift_right_logical(i + 1, 1)
        return jnp.where((i & 1) == 1, half, mod(SIDE - half, SIDE))

    def send_chunk(dx):
        @pl.loop(0, SIDE, unroll=4)
        def _(yo):
            owner = mod(x + dx, SIDE) * SIDE + yo
            near = mod(yo - y + SIDE, SIDE) < SIDE // 2
            kind = jnp.where(near, 0, 1)
            dest = jnp.where(near, owner, mod(owner + 1, n))

            @pl.when(dest != me)
            def _():
                pltpu.make_async_remote_copy(
                    src_ref=msgs.at[owner],
                    dst_ref=raw.at[kind, me],
                    send_sem=sent_sem.at[0],
                    recv_sem=direct_sem.at[kind, dx],
                    device_id={"genes": dest},
                    device_id_type=MESH,
                ).start()

            @pl.when(dest == me)
            def _():
                pltpu.make_async_copy(
                    msgs.at[owner], raw.at[kind, me], direct_sem.at[kind, dx]
                ).start()

    for load in loads:
        load.wait()
    with jax.named_scope("permute"):
        for t in range(counts_flat.shape[1] // ALIGN):
            counts_ref[t] = counts_flat[:, t * ALIGN : (t + 1) * ALIGN]
        counts_ref[counts_ref.shape[0] - 1] = counts_flat[:, :ALIGN]

        @pl.loop(0, n, unroll=8)
        def _(owner):
            permuted(counts_ref, block_ref, msgs, owner)

    with jax.named_scope("barrier"):
        pl.semaphore_wait(barrier, n)
    expr_copy = pltpu.make_async_remote_copy(
        src_ref=expr_ref,
        dst_ref=expr.at[1],
        send_sem=expr_sem.at[0],
        recv_sem=expr_sem.at[1],
        device_id={"genes": nxt},
        device_id_type=MESH,
    )
    expr_copy.start()
    with jax.named_scope("send"):

        @pl.loop(0, SIDE)
        def _(i):
            send_chunk(chunk(i))

    dose_copy = pltpu.make_async_remote_copy(
        src_ref=dose_ref,
        dst_ref=dose.at[1],
        send_sem=dose_sem.at[0],
        recv_sem=dose_sem.at[1],
        device_id={"samples": other},
        device_id_type=MESH,
    )
    dose_copy.start()
    with jax.named_scope("keys"):
        for kind, owner in enumerate((me, prv)):
            membership(sizes_ref, mask_ref, owner, sd.at[kind])
    mine.wait()

    def dose_squares(slot, first, rows):
        for r in range(rows // ALIGN):
            at = pl.ds(pl.multiple_of(first + r * ALIGN, ALIGN), ALIGN)
            square = jnp.zeros((ALIGN, ALIGN), jnp.float32) if slot == 0 else squares[at]
            for k in range(HALF // ALIGN):
                value = dose[slot, at, k * ALIGN : (k + 1) * ALIGN].astype(jnp.float32)
                square = square + value * value
            squares[at] = square

    def relay_chunk(dx):
        for kind in range(2):
            pltpu.make_async_copy(
                raw.at[kind, 0 : SIDE // 2], raw.at[kind, 0 : SIDE // 2], direct_sem.at[kind, dx]
            ).wait()
        for kind, partner in ((0, nxt), (1, prv)):
            xs = mod((x if kind == 0 else xp) + SIDE - dx, SIDE)

            @pl.loop(0, SIDE // 2)
            def _(t):
                ys = mod(y + SIDE - t, SIDE) if kind == 0 else mod(y + t, SIDE)
                source = xs * SIDE + ys
                pltpu.make_async_remote_copy(
                    src_ref=raw.at[kind, source],
                    dst_ref=raw.at[1 - kind, source],
                    send_sem=sent_sem.at[1],
                    recv_sem=relay_sem.at[1 - kind, dx],
                    device_id={"genes": partner},
                    device_id_type=MESH,
                ).start()

    def ratio_chunk(dx):
        for kind in range(2):
            pltpu.make_async_copy(
                raw.at[kind, 0 : SIDE // 2], raw.at[kind, 0 : SIDE // 2], relay_sem.at[kind, dx]
            ).wait()
            xs = mod((x if kind == 0 else xp) + SIDE - dx, SIDE)
            at = pl.ds(xs * SIDE, SIDE)
            low = raw[kind, at, :16].reshape(ALIGN, ALIGN)
            high = raw[kind, at, 16:32].reshape(ALIGN, ALIGN)
            left = raw[kind, at, 32:].astype(jnp.float32)
            right = pltpu.roll(left, ALIGN // 2, 2)
            last = jnp.concatenate([left, right], axis=1).reshape(ALIGN, ALIGN).astype(jnp.bfloat16)
            counts = jnp.concatenate([low, high, last], axis=1)
            both = lax.dot_general(sd[kind], counts, NT, preferred_element_type=jnp.float32)
            ratio = both[RATIOS:] / jnp.maximum(both[:RATIOS], 1.0)
            own = expr[kind, :, pl.ds(pl.multiple_of(xs * ALIGN, ALIGN), ALIGN)].astype(jnp.float32)
            rest = jnp.ones((ROWS - USED, ALIGN), jnp.float32)
            panel[kind, 0, xs] = jnp.concatenate([own, ratio, rest], axis=0).astype(jnp.bfloat16)

    def panel_copy(kind, dx):
        xs = mod((x if kind == 0 else xp) + SIDE - dx, SIDE)
        return pltpu.make_async_remote_copy(
            src_ref=panel.at[kind, 0, xs],
            dst_ref=panel.at[kind, 1, xs],
            send_sem=panel_sem.at[kind, 0],
            recv_sem=panel_sem.at[kind, 1],
            device_id={"samples": other},
            device_id_type=MESH,
        )

    def panel_chunk(dx):
        panel_copy(0, dx).start()

        @pl.when(core == 0)
        def _():
            panel_copy(1, dx).start()

    def pass_on(i, slot=None):
        if slot is not None:
            with jax.named_scope("squares"):
                dose_squares(slot, i * 512, 512)
        with jax.named_scope("relay"):
            relay_chunk(chunk(i))

    @pl.loop(0, SIDE // 2)
    def _(i):
        pass_on(i, 0)

    @pl.loop(SIDE // 2, SIDE)
    def _(i):
        pass_on(i)

    with jax.named_scope("dose_wait"):
        dose_copy.wait_recv()
    with jax.named_scope("squares_1"):

        @pl.loop(0, W // 512)
        def _(i):
            dose_squares(1, i * 512, 512)

    count = float(2 * HALF)
    with jax.named_scope("square_rows"):
        for c in range(W // 512):
            at = slice(c * 512, (c + 1) * 512)
            stat[:, at] = lax.dot_general(
                jnp.ones((8, ALIGN), jnp.float32),
                squares[at],
                NT,
                precision=lax.Precision.HIGHEST,
                preferred_element_type=jnp.float32,
            )

    expr_copy.wait()
    with jax.named_scope("ratio"):
        ratio_chunk(chunk(0))

    @pl.loop(1, SIDE)
    def _(i):
        with jax.named_scope("ratio"):
            ratio_chunk(chunk(i))
        panel_chunk(chunk(i - 1))

    def joined(kind, slot):
        return jnp.concatenate([panel[kind, slot, k] for k in range(SIDE)], axis=1)

    first_left = joined(core, 0)
    panel_chunk(chunk(SIDE - 1))
    with jax.named_scope("partial"):

        @pl.loop(0, HALF // STEP)
        def _(c):
            at = pl.multiple_of(c * STEP, STEP)
            partial[c] = lax.dot_general(
                first_left, dose[0, pl.ds(at, STEP)], NT, preferred_element_type=jnp.float32
            )

    def panel_wait(kind, way):
        pltpu.make_async_copy(panel.at[kind, 1], panel.at[kind, 1], panel_sem.at[kind, way]).wait()

    with jax.named_scope("panel_wait"):
        panel_wait(0, 1)

    @pl.when(core == 1)
    def _():
        panel_wait(1, 1)

    def pheno_stats(kind):
        PIECE = 48
        for g in range(ROWS // PIECE):
            rows = slice(g * PIECE, (g + 1) * PIECE)
            total = jnp.zeros((PIECE, ALIGN), jnp.float32)
            square = jnp.zeros((PIECE, ALIGN), jnp.float32)
            for slot in range(2):
                for k in range(SIDE):
                    value = panel[kind, slot, k, rows].astype(jnp.float32)
                    total = total + value
                    square = square + value * value
            total = jnp.sum(total, axis=1, keepdims=True)
            square = jnp.sum(square, axis=1, keepdims=True)
            pstat[0, rows] = jnp.broadcast_to(total, (PIECE, ALIGN))
            scale = lax.rsqrt(jnp.maximum(square - total * total / count, 1.0))
            pstat[1, rows] = jnp.broadcast_to(scale, (PIECE, ALIGN))

    def assoc(kind, first, to_ref, scale, after=None):
        left = joined(kind, 1)
        base = None if first == 0 else joined(kind, 0)

        @pl.loop(0, HALF // STEP)
        def _(c):
            at = pl.multiple_of(first + c * STEP, STEP)
            product = lax.dot_general(
                left, dose[1, pl.ds(at, STEP)], NT, preferred_element_type=jnp.float32
            )
            if base is None:
                product = product + partial[c]
            else:
                product = product + lax.dot_general(
                    base, dose[0, pl.ds(at, STEP)], NT, preferred_element_type=jnp.float32
                )
            if after is not None:

                @pl.when(c > 0)
                def _():
                    after(c - 1)

            for k in range(STEP // ALIGN):
                here = pl.ds(pl.multiple_of(at + k * ALIGN, ALIGN), ALIGN)
                part = product[:, k * ALIGN : (k + 1) * ALIGN]
                total = part[USED : USED + 1]
                mean = total * (1.0 / count)
                dev = lax.rsqrt(jnp.maximum(stat[0:1, here] - total * mean, 1.0)) * scale
                part = (part - pstat[0] * mean) * dev * pstat[1]
                to_ref[c * (STEP // ALIGN) + k] = part.astype(jnp.bfloat16)
        if after is not None:
            after(HALF // STEP - 1)

    keep = jnp.where(me == 0, 0.0, 1.0)

    per = STEP // ALIGN
    first_half, second_half = z_ref.at[0:SIDE], z_ref.at[SIDE : 2 * SIDE]

    def give(c):
        return pltpu.make_async_remote_copy(
            src_ref=back.at[pl.ds(c * per, per)],
            dst_ref=land.at[pl.ds(c * per, per)],
            send_sem=back_send_sem,
            recv_sem=back_sem.at[c],
            device_id={"genes": prv},
            device_id_type=MESH,
        )

    @pl.when(core == 0)
    def _():
        with jax.named_scope("pstats_a"):
            pheno_stats(0)
        with jax.named_scope("assoc_a"):
            assoc(0, 0, first_half, 1.0)
            assoc(0, HALF, second_half, 1.0)

    @pl.when(core == 1)
    def _():
        with jax.named_scope("pstats_b"):
            pheno_stats(1)
        with jax.named_scope("assoc_b"):
            assoc(1, 0, back, keep, lambda c: give(c).start())
        with jax.named_scope("assoc_c"):
            pheno_stats(0)
            assoc(0, HALF, first_half, 1.0)

    gene = lax.broadcasted_iota(jnp.int32, (ROWS, ALIGN), 0) & (GENE_DEV - 1)

    def write(c):
        to = pl.ds(pl.multiple_of(c * STEP, STEP), STEP)
        return pltpu.make_async_copy(result.at[c], out_ref.at[:, :, to], out_sem.at[c])

    with jax.named_scope("cut"):

        @pl.loop(0, HALF // STEP)
        def _(c):
            @pl.when(core == 1)
            def _():
                piece = land.at[pl.ds(c * per, per)]
                pltpu.make_async_copy(piece, piece, back_sem.at[c]).wait()
                for k in range(per):
                    z_ref[SIDE + c * per + k] = land[c * per + k]

            for k in range(per):
                part = None
                for g in range(GENE_DEV):
                    value = z_ref[lax.shift_right_logical(start_ref[g], 7) + (c * per + k)]
                    part = value if g == 0 else jnp.where(gene == g, value, part)
                result[c, :, :, k * ALIGN : (k + 1) * ALIGN] = part[:USED].reshape(
                    PHEN, GENE_DEV, ALIGN
                )

            @pl.when(c > 0)
            def _():
                write(c - 1).start()

        write(HALF // STEP - 1).start()
        for c in range(HALF // STEP):
            write(c).wait()

    @pl.when(core == 1)
    def _():
        pltpu.make_async_copy(back, back, back_send_sem).wait()

    dose_copy.wait_send()
    pltpu.make_async_copy(raw.at[0, 0 : n - 2], raw.at[0, 0 : n - 2], sent_sem.at[0]).wait()
    pltpu.make_async_copy(raw.at[0], raw.at[0], sent_sem.at[1]).wait()
    panel_wait(0, 0)

    @pl.when(core == 0)
    def _():
        panel_wait(1, 0)


def shards(dosage, expression, intron_counts, cluster_sizes, valid_mask, gene_block, window_start):
    n = lax.axis_size("genes")
    dma = pltpu.SemaphoreType.DMA
    bf16, f32 = jnp.bfloat16, jnp.float32
    out = pl.pallas_call(
        functools.partial(kernel, n),
        out_shape=jax.ShapeDtypeStruct((PHEN, GENE_DEV, HALF), bf16),
        in_specs=[pl.BlockSpec(memory_space=pl.ANY)] * 7,
        out_specs=pl.BlockSpec(memory_space=pl.ANY),
        scratch_shapes=[
            pltpu.SMEM(gene_block.shape, jnp.int32),
            pltpu.SMEM(window_start.shape, jnp.int32),
            pltpu.VMEM(cluster_sizes.shape[::-1], jnp.int32),
            pltpu.VMEM(valid_mask.shape[::-1], jnp.int32),
            pltpu.VMEM((2 * SIDE, ROWS, ALIGN), bf16),
            pltpu.VMEM(intron_counts.shape, bf16),
            pltpu.VMEM((intron_counts.shape[1] // ALIGN + 1, 16, ALIGN), bf16),
            pltpu.VMEM((n, SLOTS, ALIGN), bf16),
            pltpu.VMEM((2, n, SLOTS, ALIGN), bf16),
            pltpu.VMEM((2, GENE_DEV, HALF), bf16),
            pltpu.VMEM((2, 2, SIDE, ROWS, ALIGN), bf16),
            pltpu.VMEM((2, W, HALF), bf16),
            pltpu.VMEM((W, ALIGN), f32),
            pltpu.VMEM((8, W), f32),
            pltpu.VMEM((2, ROWS, ALIGN), f32),
            pltpu.VMEM((2, 2 * RATIOS, LANES), bf16),
            pltpu.VMEM((SIDE, ROWS, ALIGN), bf16),
            pltpu.VMEM((SIDE, ROWS, ALIGN), bf16),
            pltpu.VMEM((HALF // STEP, ROWS, STEP), f32),
            pltpu.VMEM((HALF // STEP, PHEN, GENE_DEV, STEP), bf16),
            dma((2, SIDE)),
            dma((2, SIDE)),
            dma((2, 2)),
            dma((2,)),
            dma,
            dma((2,)),
            dma((2,)),
            dma((HALF // STEP,)),
            dma,
            dma((HALF // STEP,)),
            dma((6,)),
        ],
        compiler_params=pltpu.CompilerParams(collective_id=0, has_side_effects=True),
        name="associate",
    )(
        gene_block,
        window_start,
        intron_counts,
        expression,
        cluster_sizes.T,
        valid_mask.T,
        dosage,
    )
    return jnp.swapaxes(out, 0, 1)


def solution(mesh):
    in_specs = (
        P(("parts", "genes"), "samples"),
        P(("parts", "genes"), "samples"),
        P(("parts", "samples", "genes"), None),
        P("parts", None),
        P("parts", None),
        P("parts"),
        P(("parts", "genes")),
    )
    out_specs = P(("parts", "genes"), None, "samples")
    return jax.shard_map(shards, mesh=mesh, in_specs=in_specs, out_specs=out_specs, check_vma=False)
```

```python
import functools

import jax
import jax.numpy as jnp
from jax import lax
from jax.experimental import pallas as pl
from jax.experimental.pallas import tpu as pltpu
from jax.sharding import PartitionSpec as P

W = 2048
HALF = 1024
SLOTS = 40
ALIGN = 128
PHEN = 41
ROWS = 336
USED = 328
RATIOS = 320
STEP = 256
GENE_DEV = 8
LANES = 384
SIDE = 8
MESH = pl.DeviceIdType.MESH
NT = (((1,), (1,)), ((), ()))


def mod(value, size):
    return value & (size - 1) if size & (size - 1) == 0 else lax.rem(value, size)


def permuted(counts_ref, block_ref, msgs_ref, owner):
    lane = lax.broadcasted_iota(jnp.int32, (16, ALIGN), 1)
    tiles = [None] * 3
    for j in range(GENE_DEV):
        first = block_ref[owner * GENE_DEV + j] * SLOTS
        tile = lax.shift_right_logical(first, 7)
        start = first & (ALIGN - 1)
        a = counts_ref[tile].astype(jnp.float32)
        b = counts_ref[tile + 1].astype(jnp.float32)
        q = j * SLOTS % ALIGN
        gene = pltpu.roll(jnp.where(lane >= start, a, b), (q - start) & (ALIGN - 1), 1)
        t = j * SLOTS // ALIGN
        tiles[t] = gene if q == 0 else jnp.where(lane >= q, gene, tiles[t])
        if q + SLOTS > ALIGN:
            tiles[t + 1] = gene
    packed = jnp.where(lane[:8] < ALIGN // 2, tiles[2][:8], pltpu.roll(tiles[2][8:], ALIGN // 2, 1))
    msgs_ref[owner] = jnp.concatenate([tiles[0], tiles[1], packed], axis=0).astype(jnp.bfloat16)


def membership(sizes_ref, mask_ref, owner, sd_ref):
    per = ALIGN // GENE_DEV
    at = pl.ds(pl.multiple_of(owner // per * ALIGN, ALIGN), ALIGN)
    turn = (ALIGN - owner % per * GENE_DEV) % ALIGN
    sizes = pltpu.roll(sizes_ref[:, at].astype(jnp.float32), turn, 1)
    mask = pltpu.roll(mask_ref[:, at].astype(jnp.float32), turn, 1)
    slot = lax.broadcasted_iota(jnp.int32, (SLOTS, ALIGN), 0).astype(jnp.float32)
    ends = jnp.zeros((1, ALIGN), jnp.float32)
    cluster = jnp.zeros((SLOTS, ALIGN), jnp.float32)
    for c in range(8):
        ends = ends + sizes[c : c + 1]
        cluster = cluster + (ends <= slot).astype(jnp.float32)

    gene = lax.broadcasted_iota(jnp.int32, (SLOTS, GENE_DEV, ALIGN), 1)
    lane = lax.broadcasted_iota(jnp.int32, (SLOTS, GENE_DEV, ALIGN), 2)
    key = jnp.where(lane == gene, cluster[:, None, :], 0.0)
    key = jnp.sum(key, axis=2, keepdims=True).reshape(RATIOS, 1)
    row = lax.broadcasted_iota(jnp.int32, (RATIOS, 1), 0)
    row_gene = row & (GENE_DEV - 1)
    row_slot = lax.shift_right_logical(row, 3)
    row_key = key + (row_gene * 16).astype(jnp.float32)
    row_spot = row_gene * SLOTS + row_slot

    spot = lax.broadcasted_iota(jnp.int32, (ALIGN, LANES), 1)
    spot_gene = sum((spot >= SLOTS * g).astype(jnp.int32) for g in range(1, GENE_DEV + 1))
    pick = (lax.broadcasted_iota(jnp.int32, (ALIGN, LANES), 0) == spot_gene).astype(jnp.float32)
    spot, spot_gene = spot[:SLOTS], spot_gene[:SLOTS]
    here = lax.broadcasted_iota(jnp.int32, (SLOTS, LANES), 0) == spot - spot_gene * SLOTS

    def laid(value):
        full = lax.dot_general(
            value,
            pick,
            (((1,), (0,)), ((), ())),
            precision=lax.Precision.HIGHEST,
            preferred_element_type=jnp.float32,
        )
        return jnp.sum(jnp.where(here, full, 0.0), axis=0, keepdims=True)

    live = (laid(mask) > 0.5) & (spot[:1] < RATIOS)
    lane_key = jnp.where(live, laid(cluster) + (spot_gene[:1] * 16).astype(jnp.float32), -1.0)
    lane_spot = jnp.where(live, spot[:1], -1)
    sd_ref[:RATIOS] = (row_key == lane_key).astype(jnp.float32).astype(jnp.bfloat16)
    sd_ref[RATIOS:] = (row_spot == lane_spot).astype(jnp.float32).astype(jnp.bfloat16)


def kernel(
    n,
    block_hbm,
    start_hbm,
    counts_hbm,
    expr_ref,
    sizes_hbm,
    mask_hbm,
    dose_ref,
    out_ref,
    block_ref,
    start_ref,
    sizes_ref,
    mask_ref,
    z_ref,
    counts_flat,
    counts_ref,
    msgs,
    raw,
    expr,
    panel,
    dose,
    squares,
    stat,
    pstat,
    sd,
    back,
    land,
    partial,
    result,
    direct_sem,
    relay_sem,
    panel_sem,
    sent_sem,
    local_sem,
    dose_sem,
    expr_sem,
    back_sem,
    back_send_sem,
    out_sem,
    load_sem,
):
    me = lax.axis_index("genes")
    core = lax.axis_index("samples")
    x, y = lax.shift_right_logical(me, 3), me & (SIDE - 1)
    nxt, prv = mod(me + 1, n), mod(me + n - 1, n)
    other = 1 - core
    xp = jnp.where(y > 0, x, mod(x + SIDE - 1, SIDE))

    loads = [
        pltpu.make_async_copy(source, to, load_sem.at[k])
        for k, (source, to) in enumerate(
            (
                (counts_hbm, counts_flat),
                (block_hbm, block_ref),
                (start_hbm, start_ref),
                (sizes_hbm, sizes_ref),
                (mask_hbm, mask_ref),
                (expr_ref, expr.at[0]),
            )
        )
    ]
    for load in loads:
        load.start()
    barrier = pltpu.get_barrier_semaphore()
    pl.semaphore_signal(barrier, inc=1, device_id={"samples": other}, device_id_type=MESH)

    @pl.loop(1, n)
    def _(step):
        pl.semaphore_signal(
            barrier, inc=1, device_id={"genes": mod(me + step, n)}, device_id_type=MESH
        )

    mine = pltpu.make_async_copy(dose_ref, dose.at[0], local_sem)
    mine.start()

    def chunk(i):
        half = lax.shift_right_logical(i + 1, 1)
        return jnp.where((i & 1) == 1, half, mod(SIDE - half, SIDE))

    def send_chunk(dx):
        @pl.loop(0, SIDE, unroll=4)
        def _(yo):
            owner = mod(x + dx, SIDE) * SIDE + yo
            near = mod(yo - y + SIDE, SIDE) < SIDE // 2
            kind = jnp.where(near, 0, 1)
            dest = jnp.where(near, owner, mod(owner + 1, n))

            @pl.when(dest != me)
            def _():
                pltpu.make_async_remote_copy(
                    src_ref=msgs.at[owner],
                    dst_ref=raw.at[kind, me],
                    send_sem=sent_sem.at[0],
                    recv_sem=direct_sem.at[kind, dx],
                    device_id={"genes": dest},
                    device_id_type=MESH,
                ).start()

            @pl.when(dest == me)
            def _():
                pltpu.make_async_copy(
                    msgs.at[owner], raw.at[kind, me], direct_sem.at[kind, dx]
                ).start()

    for load in loads:
        load.wait()
    with jax.named_scope("permute"):
        for t in range(counts_flat.shape[1] // ALIGN):
            counts_ref[t] = counts_flat[:, t * ALIGN : (t + 1) * ALIGN]
        counts_ref[counts_ref.shape[0] - 1] = counts_flat[:, :ALIGN]

        @pl.loop(0, n, unroll=8)
        def _(owner):
            permuted(counts_ref, block_ref, msgs, owner)

    with jax.named_scope("barrier"):
        pl.semaphore_wait(barrier, n)
    expr_copy = pltpu.make_async_remote_copy(
        src_ref=expr_ref,
        dst_ref=expr.at[1],
        send_sem=expr_sem.at[0],
        recv_sem=expr_sem.at[1],
        device_id={"genes": nxt},
        device_id_type=MESH,
    )
    expr_copy.start()
    with jax.named_scope("send"):

        @pl.loop(0, SIDE)
        def _(i):
            send_chunk(chunk(i))

    dose_copy = pltpu.make_async_remote_copy(
        src_ref=dose_ref,
        dst_ref=dose.at[1],
        send_sem=dose_sem.at[0],
        recv_sem=dose_sem.at[1],
        device_id={"samples": other},
        device_id_type=MESH,
    )
    dose_copy.start()
    with jax.named_scope("keys"):
        for kind, owner in enumerate((me, prv)):
            membership(sizes_ref, mask_ref, owner, sd.at[kind])
    mine.wait()

    def dose_squares(slot, first, rows):
        for r in range(rows // ALIGN):
            at = pl.ds(pl.multiple_of(first + r * ALIGN, ALIGN), ALIGN)
            square = jnp.zeros((ALIGN, ALIGN), jnp.float32) if slot == 0 else squares[at]
            for k in range(HALF // ALIGN):
                value = dose[slot, at, k * ALIGN : (k + 1) * ALIGN].astype(jnp.float32)
                square = square + value * value
            squares[at] = square

    def column(kind, dx):
        return mod((x if kind == 0 else xp) + SIDE - dx, SIDE)

    def relay_chunk(dx):
        for kind in range(2):
            pltpu.make_async_copy(
                raw.at[kind, 0 : SIDE // 2], raw.at[kind, 0 : SIDE // 2], direct_sem.at[kind, dx]
            ).wait()
        for kind, partner in ((0, nxt), (1, prv)):
            xs = column(kind, dx)

            @pl.loop(0, SIDE // 2)
            def _(t):
                ys = mod(y + SIDE - t, SIDE) if kind == 0 else mod(y + t, SIDE)
                source = xs * SIDE + ys
                pltpu.make_async_remote_copy(
                    src_ref=raw.at[kind, source],
                    dst_ref=raw.at[1 - kind, source],
                    send_sem=sent_sem.at[1],
                    recv_sem=relay_sem.at[1 - kind, dx],
                    device_id={"genes": partner},
                    device_id_type=MESH,
                ).start()

    def slots_of(kind, xs):
        at = pl.ds(xs * SIDE, SIDE)
        low = raw[kind, at, :16].reshape(ALIGN, ALIGN)
        high = raw[kind, at, 16:32].reshape(ALIGN, ALIGN)
        left = raw[kind, at, 32:].astype(jnp.float32)
        right = pltpu.roll(left, ALIGN // 2, 2)
        last = jnp.concatenate([left, right], axis=1).reshape(ALIGN, ALIGN).astype(jnp.bfloat16)
        return jnp.concatenate([low, high, last], axis=1)

    def ratio_pair(p):
        pair = (chunk(2 * p), chunk(2 * p + 1))
        for dx in pair:
            for kind in range(2):
                part = raw.at[kind, 0 : SIDE // 2]
                pltpu.make_async_copy(part, part, relay_sem.at[kind, dx]).wait()
        for kind in range(2):
            columns = [column(kind, dx) for dx in pair]
            counts = jnp.concatenate([slots_of(kind, xs) for xs in columns], axis=0)
            both = lax.dot_general(sd[kind], counts, NT, preferred_element_type=jnp.float32)
            ratio = both[RATIOS:] / jnp.maximum(both[:RATIOS], 1.0)
            rest = jnp.ones((ROWS - USED, ALIGN), jnp.float32)
            for k, xs in enumerate(columns):
                own = expr[kind, :, pl.ds(pl.multiple_of(xs * ALIGN, ALIGN), ALIGN)].astype(jnp.float32)
                part = ratio[:, k * ALIGN : (k + 1) * ALIGN]
                panel[kind, 0, xs] = jnp.concatenate([own, part, rest], axis=0).astype(jnp.bfloat16)

    def panel_copy(kind, dx):
        xs = column(kind, dx)
        return pltpu.make_async_remote_copy(
            src_ref=panel.at[kind, 0, xs],
            dst_ref=panel.at[kind, 1, xs],
            send_sem=panel_sem.at[kind, 0],
            recv_sem=panel_sem.at[kind, 1],
            device_id={"samples": other},
            device_id_type=MESH,
        )

    def panel_chunk(dx):
        panel_copy(0, dx).start()

        @pl.when(core == 0)
        def _():
            panel_copy(1, dx).start()

    def pass_on(i, slot=None):
        if slot is not None:
            with jax.named_scope("squares"):
                dose_squares(slot, i * 512, 512)
        with jax.named_scope("relay"):
            relay_chunk(chunk(i))

    @pl.loop(0, SIDE // 2)
    def _(i):
        pass_on(i, 0)

    expr_copy.wait()

    def pair_out(p):
        panel_chunk(chunk(2 * p))
        panel_chunk(chunk(2 * p + 1))

    @pl.loop(2, SIDE // 2)
    def _(p):
        pass_on(2 * p)
        pass_on(2 * p + 1)
        with jax.named_scope("ratio"):
            ratio_pair(p - 2)

    pair_out(0)
    pair_out(1)
    for p in (2, 3):
        with jax.named_scope("ratio_end"):
            ratio_pair(p)
        if p > 2:
            pair_out(p - 1)

    def joined(kind, slot):
        return jnp.concatenate([panel[kind, slot, k] for k in range(SIDE)], axis=1)

    first_left = joined(core, 0)
    pair_out(SIDE // 2 - 1)
    with jax.named_scope("partial"):

        @pl.loop(0, HALF // STEP)
        def _(c):
            at = pl.multiple_of(c * STEP, STEP)
            partial[c] = lax.dot_general(
                first_left, dose[0, pl.ds(at, STEP)], NT, preferred_element_type=jnp.float32
            )

    with jax.named_scope("dose_wait"):
        dose_copy.wait_recv()
    with jax.named_scope("squares_1"):

        @pl.loop(0, W // 512)
        def _(i):
            dose_squares(1, i * 512, 512)

    count = float(2 * HALF)
    with jax.named_scope("square_rows"):
        for c in range(W // 512):
            at = slice(c * 512, (c + 1) * 512)
            stat[:, at] = lax.dot_general(
                jnp.ones((8, ALIGN), jnp.float32),
                squares[at],
                NT,
                precision=lax.Precision.HIGHEST,
                preferred_element_type=jnp.float32,
            )

    def panel_wait(kind, way):
        pltpu.make_async_copy(panel.at[kind, 1], panel.at[kind, 1], panel_sem.at[kind, way]).wait()

    with jax.named_scope("panel_wait"):
        panel_wait(0, 1)

    @pl.when(core == 1)
    def _():
        panel_wait(1, 1)

    def pheno_stats(kind):
        PIECE = 48
        for g in range(ROWS // PIECE):
            rows = slice(g * PIECE, (g + 1) * PIECE)
            total = jnp.zeros((PIECE, ALIGN), jnp.float32)
            square = jnp.zeros((PIECE, ALIGN), jnp.float32)
            for slot in range(2):
                for k in range(SIDE):
                    value = panel[kind, slot, k, rows].astype(jnp.float32)
                    total = total + value
                    square = square + value * value
            total = jnp.sum(total, axis=1, keepdims=True)
            square = jnp.sum(square, axis=1, keepdims=True)
            pstat[0, rows] = jnp.broadcast_to(total, (PIECE, ALIGN))
            scale = lax.rsqrt(jnp.maximum(square - total * total / count, 1.0))
            pstat[1, rows] = jnp.broadcast_to(scale, (PIECE, ALIGN))

    def assoc(kind, first, to_ref, scale, after=None):
        left = joined(kind, 1)
        base = None if first == 0 else joined(kind, 0)

        @pl.loop(0, HALF // STEP)
        def _(c):
            at = pl.multiple_of(first + c * STEP, STEP)
            product = lax.dot_general(
                left, dose[1, pl.ds(at, STEP)], NT, preferred_element_type=jnp.float32
            )
            if base is None:
                product = product + partial[c]
            else:
                product = product + lax.dot_general(
                    base, dose[0, pl.ds(at, STEP)], NT, preferred_element_type=jnp.float32
                )
            if after is not None:

                @pl.when(c > 0)
                def _():
                    after(c - 1)

            for k in range(STEP // ALIGN):
                here = pl.ds(pl.multiple_of(at + k * ALIGN, ALIGN), ALIGN)
                part = product[:, k * ALIGN : (k + 1) * ALIGN]
                total = part[USED : USED + 1]
                mean = total * (1.0 / count)
                dev = lax.rsqrt(jnp.maximum(stat[0:1, here] - total * mean, 1.0)) * scale
                part = (part - pstat[0] * mean) * dev * pstat[1]
                to_ref[c * (STEP // ALIGN) + k] = part.astype(jnp.bfloat16)
        if after is not None:
            after(HALF // STEP - 1)

    keep = jnp.where(me == 0, 0.0, 1.0)

    per = STEP // ALIGN
    first_half, second_half = z_ref.at[0:SIDE], z_ref.at[SIDE : 2 * SIDE]

    def give(c):
        return pltpu.make_async_remote_copy(
            src_ref=back.at[pl.ds(c * per, per)],
            dst_ref=land.at[pl.ds(c * per, per)],
            send_sem=back_send_sem,
            recv_sem=back_sem.at[c],
            device_id={"genes": prv},
            device_id_type=MESH,
        )

    @pl.when(core == 0)
    def _():
        with jax.named_scope("pstats_a"):
            pheno_stats(0)
        with jax.named_scope("assoc_a"):
            assoc(0, 0, first_half, 1.0)
            assoc(0, HALF, second_half, 1.0)

    @pl.when(core == 1)
    def _():
        with jax.named_scope("pstats_b"):
            pheno_stats(1)
        with jax.named_scope("assoc_b"):
            assoc(1, 0, back, keep, lambda c: give(c).start())
        with jax.named_scope("assoc_c"):
            pheno_stats(0)
            assoc(0, HALF, first_half, 1.0)

    gene = lax.broadcasted_iota(jnp.int32, (ROWS, ALIGN), 0) & (GENE_DEV - 1)

    def write(c):
        to = pl.ds(pl.multiple_of(c * STEP, STEP), STEP)
        return pltpu.make_async_copy(result.at[c], out_ref.at[:, :, to], out_sem.at[c])

    with jax.named_scope("cut"):

        @pl.loop(0, HALF // STEP)
        def _(c):
            @pl.when(core == 1)
            def _():
                piece = land.at[pl.ds(c * per, per)]
                pltpu.make_async_copy(piece, piece, back_sem.at[c]).wait()
                for k in range(per):
                    z_ref[SIDE + c * per + k] = land[c * per + k]

            for k in range(per):
                part = None
                for g in range(GENE_DEV):
                    value = z_ref[lax.shift_right_logical(start_ref[g], 7) + (c * per + k)]
                    part = value if g == 0 else jnp.where(gene == g, value, part)
                result[c, :, :, k * ALIGN : (k + 1) * ALIGN] = part[:USED].reshape(
                    PHEN, GENE_DEV, ALIGN
                )

            @pl.when(c > 0)
            def _():
                write(c - 1).start()

        write(HALF // STEP - 1).start()
        for c in range(HALF // STEP):
            write(c).wait()

    @pl.when(core == 1)
    def _():
        pltpu.make_async_copy(back, back, back_send_sem).wait()

    dose_copy.wait_send()
    pltpu.make_async_copy(raw.at[0, 0 : n - 2], raw.at[0, 0 : n - 2], sent_sem.at[0]).wait()
    pltpu.make_async_copy(raw.at[0], raw.at[0], sent_sem.at[1]).wait()
    panel_wait(0, 0)

    @pl.when(core == 0)
    def _():
        panel_wait(1, 0)


def shards(dosage, expression, intron_counts, cluster_sizes, valid_mask, gene_block, window_start):
    n = lax.axis_size("genes")
    dma = pltpu.SemaphoreType.DMA
    bf16, f32 = jnp.bfloat16, jnp.float32
    out = pl.pallas_call(
        functools.partial(kernel, n),
        out_shape=jax.ShapeDtypeStruct((PHEN, GENE_DEV, HALF), bf16),
        in_specs=[pl.BlockSpec(memory_space=pl.ANY)] * 7,
        out_specs=pl.BlockSpec(memory_space=pl.ANY),
        scratch_shapes=[
            pltpu.SMEM(gene_block.shape, jnp.int32),
            pltpu.SMEM(window_start.shape, jnp.int32),
            pltpu.VMEM(cluster_sizes.shape[::-1], jnp.int32),
            pltpu.VMEM(valid_mask.shape[::-1], jnp.int32),
            pltpu.VMEM((2 * SIDE, ROWS, ALIGN), bf16),
            pltpu.VMEM(intron_counts.shape, bf16),
            pltpu.VMEM((intron_counts.shape[1] // ALIGN + 1, 16, ALIGN), bf16),
            pltpu.VMEM((n, SLOTS, ALIGN), bf16),
            pltpu.VMEM((2, n, SLOTS, ALIGN), bf16),
            pltpu.VMEM((2, GENE_DEV, HALF), bf16),
            pltpu.VMEM((2, 2, SIDE, ROWS, ALIGN), bf16),
            pltpu.VMEM((2, W, HALF), bf16),
            pltpu.VMEM((W, ALIGN), f32),
            pltpu.VMEM((8, W), f32),
            pltpu.VMEM((2, ROWS, ALIGN), f32),
            pltpu.VMEM((2, 2 * RATIOS, LANES), bf16),
            pltpu.VMEM((SIDE, ROWS, ALIGN), bf16),
            pltpu.VMEM((SIDE, ROWS, ALIGN), bf16),
            pltpu.VMEM((HALF // STEP, ROWS, STEP), f32),
            pltpu.VMEM((HALF // STEP, PHEN, GENE_DEV, STEP), bf16),
            dma((2, SIDE)),
            dma((2, SIDE)),
            dma((2, 2)),
            dma((2,)),
            dma,
            dma((2,)),
            dma((2,)),
            dma((HALF // STEP,)),
            dma,
            dma((HALF // STEP,)),
            dma((6,)),
        ],
        compiler_params=pltpu.CompilerParams(collective_id=0, has_side_effects=True),
        name="associate",
    )(
        gene_block,
        window_start,
        intron_counts,
        expression,
        cluster_sizes.T,
        valid_mask.T,
        dosage,
    )
    return jnp.swapaxes(out, 0, 1)


def solution(mesh):
    in_specs = (
        P(("parts", "genes"), "samples"),
        P(("parts", "genes"), "samples"),
        P(("parts", "samples", "genes"), None),
        P("parts", None),
        P("parts", None),
        P("parts"),
        P(("parts", "genes")),
    )
    out_specs = P(("parts", "genes"), None, "samples")
    return jax.shard_map(shards, mesh=mesh, in_specs=in_specs, out_specs=out_specs, check_vma=False)
```

```python
import functools

import jax
import jax.numpy as jnp
from jax import lax
from jax.experimental import pallas as pl
from jax.experimental.pallas import tpu as pltpu
from jax.sharding import PartitionSpec as P

W = 2048
HALF = 1024
SLOTS = 40
ALIGN = 128
PHEN = 41
ROWS = 336
USED = 328
RATIOS = 320
STEP = 256
GENE_DEV = 8
LANES = 384
SIDE = 8
MESH = pl.DeviceIdType.MESH
NT = (((1,), (1,)), ((), ()))


def mod(value, size):
    return value & (size - 1) if size & (size - 1) == 0 else lax.rem(value, size)


def permuted(counts_ref, block_ref, msgs_ref, owner):
    lane = lax.broadcasted_iota(jnp.int32, (16, ALIGN), 1)
    tiles = [None] * 3
    for j in range(GENE_DEV):
        first = block_ref[owner * GENE_DEV + j] * SLOTS
        tile = lax.shift_right_logical(first, 7)
        start = first & (ALIGN - 1)
        a = counts_ref[tile].astype(jnp.float32)
        b = counts_ref[tile + 1].astype(jnp.float32)
        q = j * SLOTS % ALIGN
        gene = pltpu.roll(jnp.where(lane >= start, a, b), (q - start) & (ALIGN - 1), 1)
        t = j * SLOTS // ALIGN
        tiles[t] = gene if q == 0 else jnp.where(lane >= q, gene, tiles[t])
        if q + SLOTS > ALIGN:
            tiles[t + 1] = gene
    packed = jnp.where(lane[:8] < ALIGN // 2, tiles[2][:8], pltpu.roll(tiles[2][8:], ALIGN // 2, 1))
    msgs_ref[owner] = jnp.concatenate([tiles[0], tiles[1], packed], axis=0).astype(jnp.bfloat16)


def membership(sizes_ref, mask_ref, owner, sd_ref):
    per = ALIGN // GENE_DEV
    at = pl.ds(pl.multiple_of(owner // per * ALIGN, ALIGN), ALIGN)
    turn = (ALIGN - owner % per * GENE_DEV) % ALIGN
    sizes = pltpu.roll(sizes_ref[:, at].astype(jnp.float32), turn, 1)
    mask = pltpu.roll(mask_ref[:, at].astype(jnp.float32), turn, 1)
    slot = lax.broadcasted_iota(jnp.int32, (SLOTS, ALIGN), 0).astype(jnp.float32)
    ends = jnp.zeros((1, ALIGN), jnp.float32)
    cluster = jnp.zeros((SLOTS, ALIGN), jnp.float32)
    for c in range(8):
        ends = ends + sizes[c : c + 1]
        cluster = cluster + (ends <= slot).astype(jnp.float32)

    gene = lax.broadcasted_iota(jnp.int32, (SLOTS, GENE_DEV, ALIGN), 1)
    lane = lax.broadcasted_iota(jnp.int32, (SLOTS, GENE_DEV, ALIGN), 2)
    key = jnp.where(lane == gene, cluster[:, None, :], 0.0)
    key = jnp.sum(key, axis=2, keepdims=True).reshape(RATIOS, 1)
    row = lax.broadcasted_iota(jnp.int32, (RATIOS, 1), 0)
    row_gene = row & (GENE_DEV - 1)
    row_slot = lax.shift_right_logical(row, 3)
    row_key = key + (row_gene * 16).astype(jnp.float32)
    row_spot = row_gene * SLOTS + row_slot

    spot = lax.broadcasted_iota(jnp.int32, (ALIGN, LANES), 1)
    spot_gene = sum((spot >= SLOTS * g).astype(jnp.int32) for g in range(1, GENE_DEV + 1))
    pick = (lax.broadcasted_iota(jnp.int32, (ALIGN, LANES), 0) == spot_gene).astype(jnp.float32)
    spot, spot_gene = spot[:SLOTS], spot_gene[:SLOTS]
    here = lax.broadcasted_iota(jnp.int32, (SLOTS, LANES), 0) == spot - spot_gene * SLOTS

    def laid(value):
        full = lax.dot_general(
            value,
            pick,
            (((1,), (0,)), ((), ())),
            precision=lax.Precision.HIGHEST,
            preferred_element_type=jnp.float32,
        )
        return jnp.sum(jnp.where(here, full, 0.0), axis=0, keepdims=True)

    live = (laid(mask) > 0.5) & (spot[:1] < RATIOS)
    lane_key = jnp.where(live, laid(cluster) + (spot_gene[:1] * 16).astype(jnp.float32), -1.0)
    lane_spot = jnp.where(live, spot[:1], -1)
    sd_ref[:RATIOS] = (row_key == lane_key).astype(jnp.float32).astype(jnp.bfloat16)
    sd_ref[RATIOS:] = (row_spot == lane_spot).astype(jnp.float32).astype(jnp.bfloat16)


def kernel(
    n,
    block_hbm,
    start_hbm,
    counts_hbm,
    expr_ref,
    sizes_hbm,
    mask_hbm,
    dose_ref,
    out_ref,
    block_ref,
    start_ref,
    sizes_ref,
    mask_ref,
    z_ref,
    counts_flat,
    counts_ref,
    msgs,
    raw,
    expr,
    panel,
    dose,
    squares,
    stat,
    pstat,
    sd,
    back,
    land,
    partial,
    result,
    direct_sem,
    relay_sem,
    panel_sem,
    sent_sem,
    local_sem,
    dose_sem,
    expr_sem,
    back_sem,
    back_send_sem,
    out_sem,
    load_sem,
):
    me = lax.axis_index("genes")
    core = lax.axis_index("samples")
    x, y = lax.shift_right_logical(me, 3), me & (SIDE - 1)
    nxt, prv = mod(me + 1, n), mod(me + n - 1, n)
    other = 1 - core
    inside = (y == 1) | (y == SIDE - 2)
    xp = jnp.where(y > 0, x, mod(x + SIDE - 1, SIDE))

    loads = [
        pltpu.make_async_copy(source, to, load_sem.at[k])
        for k, (source, to) in enumerate(
            (
                (counts_hbm, counts_flat),
                (block_hbm, block_ref),
                (start_hbm, start_ref),
                (sizes_hbm, sizes_ref),
                (mask_hbm, mask_ref),
                (expr_ref, expr.at[0]),
            )
        )
    ]
    for load in loads:
        load.start()
    barrier = pltpu.get_barrier_semaphore()
    pl.semaphore_signal(barrier, inc=1, device_id={"samples": other}, device_id_type=MESH)

    @pl.loop(1, n)
    def _(step):
        pl.semaphore_signal(
            barrier, inc=1, device_id={"genes": mod(me + step, n)}, device_id_type=MESH
        )

    mine = pltpu.make_async_copy(dose_ref, dose.at[0], local_sem)
    mine.start()

    def chunk(i):
        half = lax.shift_right_logical(i + 1, 1)
        return jnp.where((i & 1) == 1, half, mod(SIDE - half, SIDE))

    def send_chunk(dx):
        @pl.loop(0, SIDE, unroll=4)
        def _(yo):
            owner = mod(x + dx, SIDE) * SIDE + yo
            near = mod(yo - y + SIDE, SIDE) < SIDE // 2
            kind = jnp.where(near, 0, 1)
            dest = jnp.where(near, owner, mod(owner + 1, n))

            @pl.when(dest != me)
            def _():
                pltpu.make_async_remote_copy(
                    src_ref=msgs.at[owner],
                    dst_ref=raw.at[kind, me],
                    send_sem=sent_sem.at[0],
                    recv_sem=direct_sem.at[kind, dx],
                    device_id={"genes": dest},
                    device_id_type=MESH,
                ).start()

            @pl.when(dest == me)
            def _():
                pltpu.make_async_copy(
                    msgs.at[owner], raw.at[kind, me], direct_sem.at[kind, dx]
                ).start()

            @pl.when((yo == SIDE - 1) & inside)
            def _():
                pltpu.make_async_remote_copy(
                    src_ref=msgs.at[owner],
                    dst_ref=raw.at[1 - kind, me],
                    send_sem=sent_sem.at[2],
                    recv_sem=relay_sem.at[1 - kind, dx],
                    device_id={"genes": jnp.where(near, mod(owner + 1, n), owner)},
                    device_id_type=MESH,
                ).start()

    for load in loads:
        load.wait()
    with jax.named_scope("permute"):
        for t in range(counts_flat.shape[1] // ALIGN):
            counts_ref[t] = counts_flat[:, t * ALIGN : (t + 1) * ALIGN]
        counts_ref[counts_ref.shape[0] - 1] = counts_flat[:, :ALIGN]

        @pl.loop(0, n, unroll=8)
        def _(owner):
            permuted(counts_ref, block_ref, msgs, owner)

    with jax.named_scope("barrier"):
        pl.semaphore_wait(barrier, n)
    expr_copy = pltpu.make_async_remote_copy(
        src_ref=expr_ref,
        dst_ref=expr.at[1],
        send_sem=expr_sem.at[0],
        recv_sem=expr_sem.at[1],
        device_id={"genes": nxt},
        device_id_type=MESH,
    )
    expr_copy.start()
    with jax.named_scope("send"):

        @pl.loop(0, SIDE)
        def _(i):
            send_chunk(chunk(i))

    dose_copy = pltpu.make_async_remote_copy(
        src_ref=dose_ref,
        dst_ref=dose.at[1],
        send_sem=dose_sem.at[0],
        recv_sem=dose_sem.at[1],
        device_id={"samples": other},
        device_id_type=MESH,
    )
    dose_copy.start()
    with jax.named_scope("keys"):
        for kind, owner in enumerate((me, prv)):
            membership(sizes_ref, mask_ref, owner, sd.at[kind])
    mine.wait()

    def dose_squares(slot, first, rows):
        for r in range(rows // ALIGN):
            at = pl.ds(pl.multiple_of(first + r * ALIGN, ALIGN), ALIGN)
            square = jnp.zeros((ALIGN, ALIGN), jnp.float32) if slot == 0 else squares[at]
            for k in range(HALF // ALIGN):
                value = dose[slot, at, k * ALIGN : (k + 1) * ALIGN].astype(jnp.float32)
                square = square + value * value
            squares[at] = square

    def column(kind, dx):
        return mod((x if kind == 0 else xp) + SIDE - dx, SIDE)

    def relay_chunk(dx):
        for kind in range(2):
            pltpu.make_async_copy(
                raw.at[kind, 0 : SIDE // 2], raw.at[kind, 0 : SIDE // 2], direct_sem.at[kind, dx]
            ).wait()
        for kind, partner in ((0, nxt), (1, prv)):
            xs = column(kind, dx)

            def send_on(t, sem):
                ys = mod(y + SIDE - t, SIDE) if kind == 0 else mod(y + t, SIDE)
                source = xs * SIDE + ys
                pltpu.make_async_remote_copy(
                    src_ref=raw.at[kind, source],
                    dst_ref=raw.at[1 - kind, source],
                    send_sem=sent_sem.at[sem],
                    recv_sem=relay_sem.at[1 - kind, dx],
                    device_id={"genes": partner},
                    device_id_type=MESH,
                ).start()

            for t in (0, 2, 3):
                send_on(t, 1)

            @pl.when(y != (SIDE - 1 if kind == 0 else 0))
            def _():
                send_on(1, 3 + kind)

    def slots_of(kind, xs):
        at = pl.ds(xs * SIDE, SIDE)
        low = raw[kind, at, :16].reshape(ALIGN, ALIGN)
        high = raw[kind, at, 16:32].reshape(ALIGN, ALIGN)
        left = raw[kind, at, 32:].astype(jnp.float32)
        right = pltpu.roll(left, ALIGN // 2, 2)
        last = jnp.concatenate([left, right], axis=1).reshape(ALIGN, ALIGN).astype(jnp.bfloat16)
        return jnp.concatenate([low, high, last], axis=1)

    def ratio_pair(p):
        pair = (chunk(2 * p), chunk(2 * p + 1))
        for dx in pair:
            for kind in range(2):
                part = raw.at[kind, 0 : SIDE // 2]
                pltpu.make_async_copy(part, part, relay_sem.at[kind, dx]).wait()
        for kind in range(2):
            columns = [column(kind, dx) for dx in pair]
            counts = jnp.concatenate([slots_of(kind, xs) for xs in columns], axis=0)
            both = lax.dot_general(sd[kind], counts, NT, preferred_element_type=jnp.float32)
            ratio = both[RATIOS:] / jnp.maximum(both[:RATIOS], 1.0)
            rest = jnp.ones((ROWS - USED, ALIGN), jnp.float32)
            for k, xs in enumerate(columns):
                own = expr[kind, :, pl.ds(pl.multiple_of(xs * ALIGN, ALIGN), ALIGN)].astype(jnp.float32)
                part = ratio[:, k * ALIGN : (k + 1) * ALIGN]
                panel[kind, 0, xs] = jnp.concatenate([own, part, rest], axis=0).astype(jnp.bfloat16)

    def panel_copy(kind, dx):
        xs = column(kind, dx)
        return pltpu.make_async_remote_copy(
            src_ref=panel.at[kind, 0, xs],
            dst_ref=panel.at[kind, 1, xs],
            send_sem=panel_sem.at[kind, 0],
            recv_sem=panel_sem.at[kind, 1],
            device_id={"samples": other},
            device_id_type=MESH,
        )

    def panel_chunk(dx):
        panel_copy(0, dx).start()

        @pl.when(core == 0)
        def _():
            panel_copy(1, dx).start()

    def pass_on(i, slot=None):
        if slot is not None:
            with jax.named_scope("squares"):
                dose_squares(slot, i * 512, 512)
        with jax.named_scope("relay"):
            relay_chunk(chunk(i))

    @pl.loop(0, SIDE // 2)
    def _(i):
        pass_on(i, 0)

    @pl.loop(SIDE // 2, SIDE)
    def _(i):
        pass_on(i)

    expr_copy.wait()

    def pair_out(p):
        panel_chunk(chunk(2 * p))
        panel_chunk(chunk(2 * p + 1))

    with jax.named_scope("ratio"):
        ratio_pair(0)
    with jax.named_scope("ratio"):
        ratio_pair(1)
    pair_out(0)
    with jax.named_scope("dose_wait"):
        dose_copy.wait_recv()
    with jax.named_scope("squares_1"):

        @pl.loop(0, W // 512)
        def _(i):
            dose_squares(1, i * 512, 512)

    pair_out(1)
    with jax.named_scope("ratio_end"):
        ratio_pair(2)
    count = float(2 * HALF)
    with jax.named_scope("square_rows"):
        for c in range(W // 512):
            at = slice(c * 512, (c + 1) * 512)
            stat[:, at] = lax.dot_general(
                jnp.ones((8, ALIGN), jnp.float32),
                squares[at],
                NT,
                precision=lax.Precision.HIGHEST,
                preferred_element_type=jnp.float32,
            )

    pair_out(2)
    with jax.named_scope("ratio_end"):
        ratio_pair(3)

    def joined(kind, slot):
        return jnp.concatenate([panel[kind, slot, k] for k in range(SIDE)], axis=1)

    first_left = joined(core, 0)
    pair_out(SIDE // 2 - 1)
    with jax.named_scope("partial"):

        @pl.loop(0, HALF // STEP)
        def _(c):
            at = pl.multiple_of(c * STEP, STEP)
            product = lax.dot_general(
                first_left, dose[0, pl.ds(at, STEP)], NT, preferred_element_type=jnp.float32
            )
            for k in range(STEP // ALIGN):
                partial[c * (STEP // ALIGN) + k] = product[:, k * ALIGN : (k + 1) * ALIGN]

    def panel_wait(kind, way):
        pltpu.make_async_copy(panel.at[kind, 1], panel.at[kind, 1], panel_sem.at[kind, way]).wait()

    with jax.named_scope("panel_wait"):
        panel_wait(0, 1)

    @pl.when(core == 1)
    def _():
        panel_wait(1, 1)

    def pheno_stats(kind):
        PIECE = 48
        for g in range(ROWS // PIECE):
            rows = slice(g * PIECE, (g + 1) * PIECE)
            total = jnp.zeros((PIECE, ALIGN), jnp.float32)
            square = jnp.zeros((PIECE, ALIGN), jnp.float32)
            for slot in range(2):
                for k in range(SIDE):
                    value = panel[kind, slot, k, rows].astype(jnp.float32)
                    total = total + value
                    square = square + value * value
            total = jnp.sum(total, axis=1, keepdims=True)
            square = jnp.sum(square, axis=1, keepdims=True)
            pstat[0, rows] = jnp.broadcast_to(total, (PIECE, ALIGN))
            scale = lax.rsqrt(jnp.maximum(square - total * total / count, 1.0))
            pstat[1, rows] = jnp.broadcast_to(scale, (PIECE, ALIGN))

    def assoc(kind, first, to_ref, scale, after=None):
        left = joined(kind, 1)
        base = None if first == 0 else joined(kind, 0)

        step = STEP if after is None else ALIGN

        @pl.loop(0, HALF // step)
        def _(c):
            at = pl.multiple_of(first + c * step, step)
            product = lax.dot_general(
                left, dose[1, pl.ds(at, step)], NT, preferred_element_type=jnp.float32
            )
            if base is not None:
                product = product + lax.dot_general(
                    base, dose[0, pl.ds(at, step)], NT, preferred_element_type=jnp.float32
                )
            if after is not None:

                @pl.when(c > 0)
                def _():
                    after(c - 1)

            for k in range(step // ALIGN):
                tile = c * (step // ALIGN) + k
                here = pl.ds(pl.multiple_of(at + k * ALIGN, ALIGN), ALIGN)
                part = product[:, k * ALIGN : (k + 1) * ALIGN]
                if base is None:
                    part = part + partial[tile]
                total = part[USED : USED + 1]
                mean = total * (1.0 / count)
                dev = lax.rsqrt(jnp.maximum(stat[0:1, here] - total * mean, 1.0)) * scale
                part = (part - pstat[0] * mean) * dev * pstat[1]
                to_ref[tile] = part.astype(jnp.bfloat16)
        if after is not None:
            after(HALF // step - 1)

    keep = jnp.where(me == 0, 0.0, 1.0)

    first_half, second_half = z_ref.at[0:SIDE], z_ref.at[SIDE : 2 * SIDE]

    def give(c):
        return pltpu.make_async_remote_copy(
            src_ref=back.at[c],
            dst_ref=land.at[c],
            send_sem=back_send_sem,
            recv_sem=back_sem.at[c],
            device_id={"genes": prv},
            device_id_type=MESH,
        )

    @pl.when(core == 0)
    def _():
        with jax.named_scope("pstats_a"):
            pheno_stats(0)
        with jax.named_scope("assoc_a"):
            assoc(0, 0, first_half, 1.0)
            assoc(0, HALF, second_half, 1.0)

    @pl.when(core == 1)
    def _():
        with jax.named_scope("pstats_b"):
            pheno_stats(1)
        with jax.named_scope("assoc_b"):
            assoc(1, 0, back, keep, lambda c: give(c).start())
        with jax.named_scope("assoc_c"):
            pheno_stats(0)
            assoc(0, HALF, first_half, 1.0)

    gene = lax.broadcasted_iota(jnp.int32, (ROWS, ALIGN), 0) & (GENE_DEV - 1)

    def write(m):
        to = pl.ds(pl.multiple_of(m * ALIGN, ALIGN), ALIGN)
        return pltpu.make_async_copy(result.at[m], out_ref.at[:, :, to], out_sem.at[m])

    with jax.named_scope("cut"):

        @pl.loop(0, SIDE)
        def _(m):
            @pl.when(core == 1)
            def _():
                pltpu.make_async_copy(land.at[m], land.at[m], back_sem.at[m]).wait()
                z_ref[SIDE + m] = land[m]

            part = None
            for g in range(GENE_DEV):
                value = z_ref[lax.shift_right_logical(start_ref[g], 7) + m]
                part = value if g == 0 else jnp.where(gene == g, value, part)
            result[m] = part[:USED].reshape(PHEN, GENE_DEV, ALIGN)

            @pl.when(m > 0)
            def _():
                write(m - 1).start()

        write(SIDE - 1).start()
        for m in range(SIDE):
            write(m).wait()

    @pl.when(core == 1)
    def _():
        pltpu.make_async_copy(back, back, back_send_sem).wait()

    dose_copy.wait_send()
    pltpu.make_async_copy(raw.at[0, 0 : n - 2], raw.at[0, 0 : n - 2], sent_sem.at[0]).wait()
    most = raw.at[0, 0 : n - 2 * SIDE]
    pltpu.make_async_copy(most, most, sent_sem.at[1]).wait()
    for sem, there in ((2, inside), (3, y != SIDE - 1), (4, y != 0)):

        @pl.when(there)
        def _():
            few = raw.at[0, 0:SIDE]
            pltpu.make_async_copy(few, few, sent_sem.at[sem]).wait()

    panel_wait(0, 0)

    @pl.when(core == 0)
    def _():
        panel_wait(1, 0)


def shards(dosage, expression, intron_counts, cluster_sizes, valid_mask, gene_block, window_start):
    n = lax.axis_size("genes")
    dma = pltpu.SemaphoreType.DMA
    bf16, f32 = jnp.bfloat16, jnp.float32
    out = pl.pallas_call(
        functools.partial(kernel, n),
        out_shape=jax.ShapeDtypeStruct((PHEN, GENE_DEV, HALF), bf16),
        in_specs=[pl.BlockSpec(memory_space=pl.ANY)] * 7,
        out_specs=pl.BlockSpec(memory_space=pl.ANY),
        scratch_shapes=[
            pltpu.SMEM(gene_block.shape, jnp.int32),
            pltpu.SMEM(window_start.shape, jnp.int32),
            pltpu.VMEM(cluster_sizes.shape[::-1], jnp.int32),
            pltpu.VMEM(valid_mask.shape[::-1], jnp.int32),
            pltpu.VMEM((2 * SIDE, ROWS, ALIGN), bf16),
            pltpu.VMEM(intron_counts.shape, bf16),
            pltpu.VMEM((intron_counts.shape[1] // ALIGN + 1, 16, ALIGN), bf16),
            pltpu.VMEM((n, SLOTS, ALIGN), bf16),
            pltpu.VMEM((2, n, SLOTS, ALIGN), bf16),
            pltpu.VMEM((2, GENE_DEV, HALF), bf16),
            pltpu.VMEM((2, 2, SIDE, ROWS, ALIGN), bf16),
            pltpu.VMEM((2, W, HALF), bf16),
            pltpu.VMEM((W, ALIGN), f32),
            pltpu.VMEM((8, W), f32),
            pltpu.VMEM((2, ROWS, ALIGN), f32),
            pltpu.VMEM((2, 2 * RATIOS, LANES), bf16),
            pltpu.VMEM((SIDE, ROWS, ALIGN), bf16),
            pltpu.VMEM((SIDE, ROWS, ALIGN), bf16),
            pltpu.VMEM((SIDE, ROWS, ALIGN), f32),
            pltpu.VMEM((SIDE, PHEN, GENE_DEV, ALIGN), bf16),
            dma((2, SIDE)),
            dma((2, SIDE)),
            dma((2, 2)),
            dma((5,)),
            dma,
            dma((2,)),
            dma((2,)),
            dma((SIDE,)),
            dma,
            dma((SIDE,)),
            dma((6,)),
        ],
        compiler_params=pltpu.CompilerParams(collective_id=0, has_side_effects=True),
        name="associate",
    )(
        gene_block,
        window_start,
        intron_counts,
        expression,
        cluster_sizes.T,
        valid_mask.T,
        dosage,
    )
    return jnp.swapaxes(out, 0, 1)


def solution(mesh):
    in_specs = (
        P(("parts", "genes"), "samples"),
        P(("parts", "genes"), "samples"),
        P(("parts", "samples", "genes"), None),
        P("parts", None),
        P("parts", None),
        P("parts"),
        P(("parts", "genes")),
    )
    out_specs = P(("parts", "genes"), None, "samples")
    return jax.shard_map(shards, mesh=mesh, in_specs=in_specs, out_specs=out_specs, check_vma=False)
```

```python
import functools

import jax
import jax.numpy as jnp
from jax import lax
from jax.experimental import pallas as pl
from jax.experimental.pallas import tpu as pltpu
from jax.sharding import PartitionSpec as P

W = 2048
HALF = 1024
SLOTS = 40
ALIGN = 128
PHEN = 41
ROWS = 336
USED = 328
RATIOS = 320
STEP = 256
GENE_DEV = 8
LANES = 384
SIDE = 8
MESH = pl.DeviceIdType.MESH
NT = (((1,), (1,)), ((), ()))


def mod(value, size):
    return value & (size - 1) if size & (size - 1) == 0 else lax.rem(value, size)


def permuted(counts_ref, block_ref, msgs_ref, owner):
    lane = lax.broadcasted_iota(jnp.int32, (16, ALIGN), 1)
    tiles = [None] * 3
    for j in range(GENE_DEV):
        first = block_ref[owner * GENE_DEV + j] * SLOTS
        tile = lax.shift_right_logical(first, 7)
        start = first & (ALIGN - 1)
        a = counts_ref[tile].astype(jnp.float32)
        b = counts_ref[tile + 1].astype(jnp.float32)
        q = j * SLOTS % ALIGN
        gene = pltpu.roll(jnp.where(lane >= start, a, b), (q - start) & (ALIGN - 1), 1)
        t = j * SLOTS // ALIGN
        tiles[t] = gene if q == 0 else jnp.where(lane >= q, gene, tiles[t])
        if q + SLOTS > ALIGN:
            tiles[t + 1] = gene
    packed = jnp.where(lane[:8] < ALIGN // 2, tiles[2][:8], pltpu.roll(tiles[2][8:], ALIGN // 2, 1))
    msgs_ref[owner] = jnp.concatenate([tiles[0], tiles[1], packed], axis=0).astype(jnp.bfloat16)


def membership(sizes_ref, mask_ref, owner, sd_ref):
    per = ALIGN // GENE_DEV
    at = pl.ds(pl.multiple_of(owner // per * ALIGN, ALIGN), ALIGN)
    turn = (ALIGN - owner % per * GENE_DEV) % ALIGN
    sizes = pltpu.roll(sizes_ref[:, at].astype(jnp.float32), turn, 1)
    mask = pltpu.roll(mask_ref[:, at].astype(jnp.float32), turn, 1)
    slot = lax.broadcasted_iota(jnp.int32, (SLOTS, ALIGN), 0).astype(jnp.float32)
    ends = jnp.zeros((1, ALIGN), jnp.float32)
    cluster = jnp.zeros((SLOTS, ALIGN), jnp.float32)
    for c in range(8):
        ends = ends + sizes[c : c + 1]
        cluster = cluster + (ends <= slot).astype(jnp.float32)

    gene = lax.broadcasted_iota(jnp.int32, (SLOTS, GENE_DEV, ALIGN), 1)
    lane = lax.broadcasted_iota(jnp.int32, (SLOTS, GENE_DEV, ALIGN), 2)
    key = jnp.where(lane == gene, cluster[:, None, :], 0.0)
    key = jnp.sum(key, axis=2, keepdims=True).reshape(RATIOS, 1)
    row = lax.broadcasted_iota(jnp.int32, (RATIOS, 1), 0)
    row_gene = row & (GENE_DEV - 1)
    row_slot = lax.shift_right_logical(row, 3)
    row_key = key + (row_gene * 16).astype(jnp.float32)
    row_spot = row_gene * SLOTS + row_slot

    spot = lax.broadcasted_iota(jnp.int32, (ALIGN, LANES), 1)
    spot_gene = sum((spot >= SLOTS * g).astype(jnp.int32) for g in range(1, GENE_DEV + 1))
    pick = (lax.broadcasted_iota(jnp.int32, (ALIGN, LANES), 0) == spot_gene).astype(jnp.float32)
    spot, spot_gene = spot[:SLOTS], spot_gene[:SLOTS]
    here = lax.broadcasted_iota(jnp.int32, (SLOTS, LANES), 0) == spot - spot_gene * SLOTS

    def laid(value):
        full = lax.dot_general(
            value,
            pick,
            (((1,), (0,)), ((), ())),
            precision=lax.Precision.HIGHEST,
            preferred_element_type=jnp.float32,
        )
        return jnp.sum(jnp.where(here, full, 0.0), axis=0, keepdims=True)

    live = (laid(mask) > 0.5) & (spot[:1] < RATIOS)
    lane_key = jnp.where(live, laid(cluster) + (spot_gene[:1] * 16).astype(jnp.float32), -1.0)
    lane_spot = jnp.where(live, spot[:1], -1)
    sd_ref[:RATIOS] = (row_key == lane_key).astype(jnp.float32).astype(jnp.bfloat16)
    sd_ref[RATIOS:] = (row_spot == lane_spot).astype(jnp.float32).astype(jnp.bfloat16)


def kernel(
    n,
    block_hbm,
    start_hbm,
    counts_hbm,
    expr_ref,
    sizes_hbm,
    mask_hbm,
    dose_ref,
    out_ref,
    block_ref,
    start_ref,
    sizes_ref,
    mask_ref,
    z_ref,
    counts_flat,
    counts_ref,
    msgs,
    raw,
    expr,
    panel,
    dose,
    squares,
    stat,
    pstat,
    sd,
    back,
    land,
    result,
    direct_sem,
    relay_sem,
    panel_sem,
    sent_sem,
    local_sem,
    dose_sem,
    expr_sem,
    back_sem,
    back_send_sem,
    out_sem,
    load_sem,
    whole_sem,
):
    me = lax.axis_index("genes")
    core = lax.axis_index("samples")
    x, y = lax.shift_right_logical(me, 3), me & (SIDE - 1)
    nxt, prv = mod(me + 1, n), mod(me + n - 1, n)
    other = 1 - core
    inside = (y == 1) | (y == SIDE - 2)
    xp = jnp.where(y > 0, x, mod(x + SIDE - 1, SIDE))

    loads = [
        pltpu.make_async_copy(source, to, load_sem.at[k])
        for k, (source, to) in enumerate(
            (
                (counts_hbm, counts_flat),
                (block_hbm, block_ref),
                (start_hbm, start_ref),
                (sizes_hbm, sizes_ref),
                (mask_hbm, mask_ref),
                (expr_ref, expr.at[0]),
            )
        )
    ]
    for load in loads:
        load.start()
    barrier = pltpu.get_barrier_semaphore()
    pl.semaphore_signal(barrier, inc=1, device_id={"samples": other}, device_id_type=MESH)

    @pl.when(core == 1)
    def _():
        pl.semaphore_signal(
            barrier, inc=1, device_id={"genes": nxt, "samples": 0}, device_id_type=MESH
        )

    @pl.loop(1, n)
    def _(step):
        pl.semaphore_signal(
            barrier, inc=1, device_id={"genes": mod(me + step, n)}, device_id_type=MESH
        )

    mine = pltpu.make_async_copy(
        dose_ref.at[pl.ds(pl.multiple_of(core * HALF, HALF), HALF)], dose.at[0], local_sem
    )
    mine.start()

    def chunk(i):
        half = lax.shift_right_logical(i + 1, 1)
        return jnp.where((i & 1) == 1, half, mod(SIDE - half, SIDE))

    def message(owner, kind, dest, send, recv):
        return pltpu.make_async_remote_copy(
            src_ref=msgs.at[owner],
            dst_ref=raw.at[kind, me],
            send_sem=sent_sem.at[send],
            recv_sem=recv,
            device_id={"genes": dest},
            device_id_type=MESH,
        )

    def send_chunk(dx):
        row = mod(x + dx, SIDE) * SIDE
        for delta in range(SIDE):
            owner = row + mod(y + delta, SIDE)
            after = mod(owner + 1, n)
            near = delta < SIDE // 2
            kind, dest, twin = (0, owner, after) if near else (1, after, owner)
            give = message(owner, kind, dest, 0, direct_sem.at[kind, dx])
            if delta in (0, SIDE - 1):

                @pl.when(dest != me)
                def _():
                    give.start()

                @pl.when(dest == me)
                def _():
                    pltpu.make_async_copy(
                        msgs.at[owner], raw.at[kind, me], direct_sem.at[kind, dx]
                    ).start()

            else:
                give.start()
            if delta in (1, SIDE - 2):

                @pl.when(y == SIDE - 1 - delta)
                def _():
                    message(owner, 1 - kind, twin, 2, relay_sem.at[1 - kind, dx]).start()

    for load in loads:
        load.wait()
    with jax.named_scope("permute"):
        for t in range(counts_flat.shape[1] // ALIGN):
            counts_ref[t] = counts_flat[:, t * ALIGN : (t + 1) * ALIGN]
        counts_ref[counts_ref.shape[0] - 1] = counts_flat[:, :ALIGN]

        @pl.loop(0, n, unroll=8)
        def _(owner):
            permuted(counts_ref, block_ref, msgs, owner)

    with jax.named_scope("barrier"):
        pl.semaphore_wait(barrier, n + 1 - core)
    expr_copy = pltpu.make_async_remote_copy(
        src_ref=expr_ref,
        dst_ref=expr.at[1],
        send_sem=expr_sem.at[0],
        recv_sem=expr_sem.at[1],
        device_id={"genes": nxt},
        device_id_type=MESH,
    )
    expr_copy.start()
    with jax.named_scope("send"):

        @pl.loop(0, SIDE)
        def _(i):
            send_chunk(chunk(i))

    dose_copy = pltpu.make_async_remote_copy(
        src_ref=dose_ref.at[pl.ds(pl.multiple_of(other * HALF, HALF), HALF)],
        dst_ref=dose.at[1],
        send_sem=dose_sem.at[0],
        recv_sem=dose_sem.at[1],
        device_id={"samples": other},
        device_id_type=MESH,
    )
    dose_copy.start()
    with jax.named_scope("keys"):
        for kind, owner in enumerate((me, prv)):
            membership(sizes_ref, mask_ref, owner, sd.at[kind])
    mine.wait()

    def dose_squares(slot, first, rows):
        for r in range(rows // ALIGN):
            at = pl.ds(pl.multiple_of(first + r * ALIGN, ALIGN), ALIGN)
            square = jnp.zeros((ALIGN, ALIGN), jnp.float32) if slot == 0 else squares[at]
            for k in range(HALF // ALIGN):
                value = dose[slot, at, k * ALIGN : (k + 1) * ALIGN].astype(jnp.float32)
                square = square + value * value
            squares[at] = square

    def column(kind, dx):
        return mod((x if kind == 0 else xp) + SIDE - dx, SIDE)

    def relay_chunk(dx):
        for kind in range(2):
            pltpu.make_async_copy(
                raw.at[kind, 0 : SIDE // 2], raw.at[kind, 0 : SIDE // 2], direct_sem.at[kind, dx]
            ).wait()
        for kind, partner in ((0, nxt), (1, prv)):
            xs = column(kind, dx)

            def send_on(t, sem):
                ys = mod(y + SIDE - t, SIDE) if kind == 0 else mod(y + t, SIDE)
                source = xs * SIDE + ys
                pltpu.make_async_remote_copy(
                    src_ref=raw.at[kind, source],
                    dst_ref=raw.at[1 - kind, source],
                    send_sem=sent_sem.at[sem],
                    recv_sem=relay_sem.at[1 - kind, dx],
                    device_id={"genes": partner},
                    device_id_type=MESH,
                ).start()

            for t in (0, 2, 3):
                send_on(t, 1)

            @pl.when(y != (SIDE - 1 if kind == 0 else 0))
            def _():
                send_on(1, 3 + kind)

    def slots_of(kind, xs):
        at = pl.ds(xs * SIDE, SIDE)
        low = raw[kind, at, :16].reshape(ALIGN, ALIGN)
        high = raw[kind, at, 16:32].reshape(ALIGN, ALIGN)
        left = raw[kind, at, 32:].astype(jnp.float32)
        right = pltpu.roll(left, ALIGN // 2, 2)
        last = jnp.concatenate([left, right], axis=1).reshape(ALIGN, ALIGN).astype(jnp.bfloat16)
        return jnp.concatenate([low, high, last], axis=1)

    def ratio_pair(p):
        pair = (chunk(2 * p), chunk(2 * p + 1))
        for dx in pair:
            for kind in range(2):
                part = raw.at[kind, 0 : SIDE // 2]
                pltpu.make_async_copy(part, part, relay_sem.at[kind, dx]).wait()
        for kind in range(2):
            columns = [column(kind, dx) for dx in pair]
            counts = jnp.concatenate([slots_of(kind, xs) for xs in columns], axis=0)
            both = lax.dot_general(sd[kind], counts, NT, preferred_element_type=jnp.float32)
            ratio = both[RATIOS:] / jnp.maximum(both[:RATIOS], 1.0)
            rest = jnp.ones((ROWS - USED, ALIGN), jnp.float32)
            for k, xs in enumerate(columns):
                own = expr[kind, :, pl.ds(pl.multiple_of(xs * ALIGN, ALIGN), ALIGN)].astype(jnp.float32)
                part = ratio[:, k * ALIGN : (k + 1) * ALIGN]
                panel[kind, 0, xs] = jnp.concatenate([own, part, rest], axis=0).astype(jnp.bfloat16)

    def panel_copy(kind, dx):
        xs = column(kind, dx)
        return pltpu.make_async_remote_copy(
            src_ref=panel.at[kind, 0, xs],
            dst_ref=panel.at[kind, 1, xs],
            send_sem=panel_sem.at[kind, 0],
            recv_sem=panel_sem.at[kind, 1],
            device_id={"samples": other},
            device_id_type=MESH,
        )

    def panel_chunk(dx):
        @pl.when(core == 1)
        def _():
            panel_copy(1, dx).start()

        panel_copy(0, dx).start()

    def pass_on(i, slot=None):
        if slot is not None:
            with jax.named_scope("squares"):
                dose_squares(slot, i * STEP, STEP)
        with jax.named_scope("relay"):
            relay_chunk(chunk(i))

    @pl.loop(0, SIDE // 2)
    def _(i):
        pass_on(i, 0)

    @pl.loop(SIDE // 2, SIDE)
    def _(i):
        pass_on(i)

    expr_copy.wait()

    def pair_out(p):
        panel_chunk(chunk(2 * p))
        panel_chunk(chunk(2 * p + 1))

    with jax.named_scope("ratio"):
        ratio_pair(0)
    with jax.named_scope("ratio"):
        ratio_pair(1)
    pair_out(0)
    with jax.named_scope("dose_wait"):
        dose_copy.wait_recv()
    with jax.named_scope("squares_1"):

        @pl.loop(0, HALF // STEP)
        def _(i):
            dose_squares(1, i * STEP, STEP)

    pair_out(1)
    with jax.named_scope("ratio_end"):
        ratio_pair(2)
    count = float(2 * HALF)
    with jax.named_scope("square_rows"):
        for c in range(HALF // 512):
            at = slice(c * 512, (c + 1) * 512)
            stat[:, at] = lax.dot_general(
                jnp.ones((8, ALIGN), jnp.float32),
                squares[at],
                NT,
                precision=lax.Precision.HIGHEST,
                preferred_element_type=jnp.float32,
            )

    pair_out(2)
    with jax.named_scope("ratio_end"):
        ratio_pair(3)

    def joined(kind, slot):
        return jnp.concatenate([panel[kind, slot, k] for k in range(SIDE)], axis=1)

    pair_out(SIDE // 2 - 1)

    PIECE = 48

    def pheno_sums(kind, slot):
        for g in range(ROWS // PIECE):
            rows = slice(g * PIECE, (g + 1) * PIECE)
            total = jnp.zeros((PIECE, ALIGN), jnp.float32) if slot == 0 else pstat[0, rows]
            square = jnp.zeros((PIECE, ALIGN), jnp.float32) if slot == 0 else pstat[1, rows]
            for k in range(SIDE):
                value = panel[kind, slot, k, rows].astype(jnp.float32)
                total = total + value
                square = square + value * value
            if slot == 1:
                total = jnp.sum(total, axis=1, keepdims=True)
                square = jnp.sum(square, axis=1, keepdims=True)
                square = lax.rsqrt(jnp.maximum(square - total * total / count, 1.0))
            pstat[0, rows] = jnp.broadcast_to(total, (PIECE, ALIGN))
            pstat[1, rows] = jnp.broadcast_to(square, (PIECE, ALIGN))

    pheno_sums(1 - core, 0)

    def panel_wait(kind, way):
        pltpu.make_async_copy(panel.at[kind, 1], panel.at[kind, 1], panel_sem.at[kind, way]).wait()

    def assoc(kind, to_ref, scale, after=None):
        left = joined(kind, 1)
        base = joined(kind, 0)

        step = STEP if after is None else ALIGN

        @pl.loop(0, HALF // step)
        def _(c):
            at = pl.multiple_of(c * step, step)
            product = lax.dot_general(
                left, dose[1, pl.ds(at, step)], NT, preferred_element_type=jnp.float32
            ) + lax.dot_general(
                base, dose[0, pl.ds(at, step)], NT, preferred_element_type=jnp.float32
            )
            if after is not None:

                @pl.when(c > 0)
                def _():
                    after(c - 1)

            for k in range(step // ALIGN):
                tile = c * (step // ALIGN) + k
                here = pl.ds(pl.multiple_of(at + k * ALIGN, ALIGN), ALIGN)
                part = product[:, k * ALIGN : (k + 1) * ALIGN]
                total = part[USED : USED + 1]
                mean = total * (1.0 / count)
                dev = lax.rsqrt(jnp.maximum(stat[0:1, here] - total * mean, 1.0)) * scale
                part = (part - pstat[0] * mean) * dev * pstat[1]
                to_ref[tile] = part.astype(jnp.bfloat16)
        if after is not None:
            after(HALF // step - 1)

    keep = jnp.where(me == 0, 0.0, 1.0)

    first_half, second_half = z_ref.at[0:SIDE], z_ref.at[SIDE : 2 * SIDE]

    def give(c):
        return pltpu.make_async_remote_copy(
            src_ref=back.at[c],
            dst_ref=land.at[c],
            send_sem=back_send_sem,
            recv_sem=back_sem.at[c],
            device_id={"genes": prv, "samples": 1},
            device_id_type=MESH,
        )

    whole = pltpu.make_async_remote_copy(
        src_ref=first_half,
        dst_ref=second_half,
        send_sem=whole_sem.at[0],
        recv_sem=whole_sem.at[1],
        device_id={"samples": 0},
        device_id_type=MESH,
    )

    @pl.when(core == 0)
    def _():
        with jax.named_scope("panel_wait"):
            panel_wait(1, 1)
        with jax.named_scope("pstats_a"):
            pheno_sums(1, 1)
        with jax.named_scope("assoc_a"):
            assoc(1, back, keep, lambda c: give(c).start())
        with jax.named_scope("assoc_b"):
            panel_wait(0, 1)
            pheno_sums(0, 0)
            pheno_sums(0, 1)
            assoc(0, first_half, 1.0)
            whole.wait_recv()

    @pl.when(core == 1)
    def _():
        with jax.named_scope("panel_wait"):
            panel_wait(0, 1)
        with jax.named_scope("pstats_b"):
            pheno_sums(0, 1)
        with jax.named_scope("assoc_c"):
            assoc(0, first_half, 1.0)
            whole.start()

    gene = lax.broadcasted_iota(jnp.int32, (ROWS, ALIGN), 0) & (GENE_DEV - 1)

    def write(m):
        to = pl.ds(pl.multiple_of(m * ALIGN, ALIGN), ALIGN)
        return pltpu.make_async_copy(result.at[m], out_ref.at[:, :, to], out_sem.at[m])

    with jax.named_scope("cut"):

        @pl.loop(0, SIDE)
        def _(m):
            @pl.when(core == 1)
            def _():
                pltpu.make_async_copy(land.at[m], land.at[m], back_sem.at[m]).wait()
                z_ref[SIDE + m] = land[m]

            part = None
            for g in range(GENE_DEV):
                value = z_ref[lax.shift_right_logical(start_ref[g], 7) + m]
                part = value if g == 0 else jnp.where(gene == g, value, part)
            result[m] = part[:USED].reshape(PHEN, GENE_DEV, ALIGN)

            @pl.when(m > 0)
            def _():
                write(m - 1).start()

        write(SIDE - 1).start()
        for m in range(SIDE):
            write(m).wait()

    @pl.when(core == 0)
    def _():
        pltpu.make_async_copy(back, back, back_send_sem).wait()

    dose_copy.wait_send()
    pltpu.make_async_copy(raw.at[0, 0 : n - 2], raw.at[0, 0 : n - 2], sent_sem.at[0]).wait()
    most = raw.at[0, 0 : n - 2 * SIDE]
    pltpu.make_async_copy(most, most, sent_sem.at[1]).wait()
    for sem, there in ((2, inside), (3, y != SIDE - 1), (4, y != 0)):

        @pl.when(there)
        def _():
            few = raw.at[0, 0:SIDE]
            pltpu.make_async_copy(few, few, sent_sem.at[sem]).wait()

    panel_wait(0, 0)

    @pl.when(core == 1)
    def _():
        whole.wait_send()
        panel_wait(1, 0)


def finish(in_ref, out_ref, held, in_sem, out_sem):
    pieces = held.shape[0]
    rows = in_ref.shape[0]
    most = held.shape[1]
    spans = [(k * most, min(most, rows - k * most)) for k in range(pieces)]
    takes = [
        pltpu.make_async_copy(in_ref.at[at : at + size], held.at[k, 0:size], in_sem.at[k])
        for k, (at, size) in enumerate(spans)
    ]
    gives = [
        pltpu.make_async_copy(held.at[k, 0:size], out_ref.at[at : at + size], out_sem.at[k])
        for k, (at, size) in enumerate(spans)
    ]
    for take in takes:
        take.start()
    for take, give in zip(takes, gives):
        take.wait()
        give.start()
    for give in gives:
        give.wait()


def shards(dosage, expression, intron_counts, cluster_sizes, valid_mask, gene_block, window_start):
    n = lax.axis_size("genes")
    dma = pltpu.SemaphoreType.DMA
    bf16, f32 = jnp.bfloat16, jnp.float32
    out = pl.pallas_call(
        functools.partial(kernel, n),
        out_shape=jax.ShapeDtypeStruct((PHEN, GENE_DEV, HALF), bf16),
        in_specs=[pl.BlockSpec(memory_space=pl.ANY)] * 7,
        out_specs=pl.BlockSpec(memory_space=pl.ANY),
        scratch_shapes=[
            pltpu.SMEM(gene_block.shape, jnp.int32),
            pltpu.SMEM(window_start.shape, jnp.int32),
            pltpu.VMEM(cluster_sizes.shape[::-1], jnp.int32),
            pltpu.VMEM(valid_mask.shape[::-1], jnp.int32),
            pltpu.VMEM((2 * SIDE, ROWS, ALIGN), bf16),
            pltpu.VMEM(intron_counts.shape, bf16),
            pltpu.VMEM((intron_counts.shape[1] // ALIGN + 1, 16, ALIGN), bf16),
            pltpu.VMEM((n, SLOTS, ALIGN), bf16),
            pltpu.VMEM((2, n, SLOTS, ALIGN), bf16),
            pltpu.VMEM((2, GENE_DEV, HALF), bf16),
            pltpu.VMEM((2, 2, SIDE, ROWS, ALIGN), bf16),
            pltpu.VMEM((2, HALF, HALF), bf16),
            pltpu.VMEM((HALF, ALIGN), f32),
            pltpu.VMEM((8, HALF), f32),
            pltpu.VMEM((2, ROWS, ALIGN), f32),
            pltpu.VMEM((2, 2 * RATIOS, LANES), bf16),
            pltpu.VMEM((SIDE, ROWS, ALIGN), bf16),
            pltpu.VMEM((SIDE, ROWS, ALIGN), bf16),
            pltpu.VMEM((SIDE, PHEN, GENE_DEV, ALIGN), bf16),
            dma((2, SIDE)),
            dma((2, SIDE)),
            dma((2, 2)),
            dma((5,)),
            dma,
            dma((2,)),
            dma((2,)),
            dma((SIDE,)),
            dma,
            dma((SIDE,)),
            dma((6,)),
            dma((2,)),
        ],
        compiler_params=pltpu.CompilerParams(collective_id=0, has_side_effects=True),
        name="associate",
    )(
        gene_block,
        window_start,
        intron_counts,
        expression,
        cluster_sizes.T,
        valid_mask.T,
        dosage,
    )
    pieces, most = 4, -(-PHEN // 4)
    out = pl.pallas_call(
        finish,
        out_shape=jax.ShapeDtypeStruct(out.shape, out.dtype),
        in_specs=[pl.BlockSpec(memory_space=pl.ANY)],
        out_specs=pl.BlockSpec(memory_space=pl.ANY),
        scratch_shapes=[pltpu.VMEM((pieces, most, GENE_DEV, HALF), bf16), dma((pieces,)), dma((pieces,))],
        name="finish",
    )(out)
    return jnp.swapaxes(out, 0, 1)


def solution(mesh):
    in_specs = (
        P(("parts", "genes"), "samples"),
        P(("parts", "genes"), "samples"),
        P(("parts", "samples", "genes"), None),
        P("parts", None),
        P("parts", None),
        P("parts"),
        P(("parts", "genes")),
    )
    out_specs = P(("parts", "genes"), None, "samples")
    return jax.shard_map(shards, mesh=mesh, in_specs=in_specs, out_specs=out_specs, check_vma=False)
```

```python
import functools

import jax
import jax.numpy as jnp
from jax import lax
from jax.experimental import pallas as pl
from jax.experimental.pallas import tpu as pltpu
from jax.sharding import PartitionSpec as P

W = 2048
HALF = 1024
SLOTS = 40
ALIGN = 128
PHEN = 41
ROWS = 336
USED = 328
RATIOS = 320
STEP = 256
GENE_DEV = 8
LANES = 384
SIDE = 8
MESH = pl.DeviceIdType.MESH
NT = (((1,), (1,)), ((), ()))


def mod(value, size):
    return value & (size - 1) if size & (size - 1) == 0 else lax.rem(value, size)


def permuted(counts_ref, block_ref, msgs_ref, owner):
    lane = lax.broadcasted_iota(jnp.int32, (16, ALIGN), 1)
    tiles = [None] * 3
    for j in range(GENE_DEV):
        first = block_ref[owner * GENE_DEV + j] * SLOTS
        tile = lax.shift_right_logical(first, 7)
        start = first & (ALIGN - 1)
        a = counts_ref[tile].astype(jnp.float32)
        b = counts_ref[tile + 1].astype(jnp.float32)
        q = j * SLOTS % ALIGN
        gene = pltpu.roll(jnp.where(lane >= start, a, b), (q - start) & (ALIGN - 1), 1)
        t = j * SLOTS // ALIGN
        tiles[t] = gene if q == 0 else jnp.where(lane >= q, gene, tiles[t])
        if q + SLOTS > ALIGN:
            tiles[t + 1] = gene
    packed = jnp.where(lane[:8] < ALIGN // 2, tiles[2][:8], pltpu.roll(tiles[2][8:], ALIGN // 2, 1))
    msgs_ref[owner] = jnp.concatenate([tiles[0], tiles[1], packed], axis=0).astype(jnp.bfloat16)


def membership(sizes_ref, mask_ref, owner, sd_ref):
    per = ALIGN // GENE_DEV
    at = pl.ds(pl.multiple_of(owner // per * ALIGN, ALIGN), ALIGN)
    turn = (ALIGN - owner % per * GENE_DEV) % ALIGN
    sizes = pltpu.roll(sizes_ref[:, at].astype(jnp.float32), turn, 1)
    mask = pltpu.roll(mask_ref[:, at].astype(jnp.float32), turn, 1)
    slot = lax.broadcasted_iota(jnp.int32, (SLOTS, ALIGN), 0).astype(jnp.float32)
    ends = jnp.zeros((1, ALIGN), jnp.float32)
    cluster = jnp.zeros((SLOTS, ALIGN), jnp.float32)
    for c in range(8):
        ends = ends + sizes[c : c + 1]
        cluster = cluster + (ends <= slot).astype(jnp.float32)

    gene = lax.broadcasted_iota(jnp.int32, (SLOTS, GENE_DEV, ALIGN), 1)
    lane = lax.broadcasted_iota(jnp.int32, (SLOTS, GENE_DEV, ALIGN), 2)
    key = jnp.where(lane == gene, cluster[:, None, :], 0.0)
    key = jnp.sum(key, axis=2, keepdims=True).reshape(RATIOS, 1)
    row = lax.broadcasted_iota(jnp.int32, (RATIOS, 1), 0)
    row_gene = row & (GENE_DEV - 1)
    row_slot = lax.shift_right_logical(row, 3)
    row_key = key + (row_gene * 16).astype(jnp.float32)
    row_spot = row_gene * SLOTS + row_slot

    spot = lax.broadcasted_iota(jnp.int32, (ALIGN, LANES), 1)
    spot_gene = sum((spot >= SLOTS * g).astype(jnp.int32) for g in range(1, GENE_DEV + 1))
    pick = (lax.broadcasted_iota(jnp.int32, (ALIGN, LANES), 0) == spot_gene).astype(jnp.float32)
    spot, spot_gene = spot[:SLOTS], spot_gene[:SLOTS]
    here = lax.broadcasted_iota(jnp.int32, (SLOTS, LANES), 0) == spot - spot_gene * SLOTS

    def laid(value):
        full = lax.dot_general(
            value,
            pick,
            (((1,), (0,)), ((), ())),
            precision=lax.Precision.HIGHEST,
            preferred_element_type=jnp.float32,
        )
        return jnp.sum(jnp.where(here, full, 0.0), axis=0, keepdims=True)

    live = (laid(mask) > 0.5) & (spot[:1] < RATIOS)
    lane_key = jnp.where(live, laid(cluster) + (spot_gene[:1] * 16).astype(jnp.float32), -1.0)
    lane_spot = jnp.where(live, spot[:1], -1)
    sd_ref[:RATIOS] = (row_key == lane_key).astype(jnp.float32).astype(jnp.bfloat16)
    sd_ref[RATIOS:] = (row_spot == lane_spot).astype(jnp.float32).astype(jnp.bfloat16)


def kernel(
    n,
    block_hbm,
    start_hbm,
    counts_hbm,
    expr_ref,
    sizes_hbm,
    mask_hbm,
    dose_ref,
    out_ref,
    block_ref,
    start_ref,
    sizes_ref,
    mask_ref,
    z_ref,
    counts_flat,
    counts_ref,
    msgs,
    raw,
    expr,
    panel,
    dose,
    squares,
    stat,
    pstat,
    sd,
    back,
    land,
    result,
    direct_sem,
    relay_sem,
    panel_sem,
    sent_sem,
    local_sem,
    dose_sem,
    expr_sem,
    back_sem,
    back_send_sem,
    out_sem,
    load_sem,
    whole_sem,
):
    me = lax.axis_index("genes")
    core = lax.axis_index("samples")
    x, y = lax.shift_right_logical(me, 3), me & (SIDE - 1)
    nxt, prv = mod(me + 1, n), mod(me + n - 1, n)
    other = 1 - core
    inside = (y == 1) | (y == SIDE - 2)
    xp = jnp.where(y > 0, x, mod(x + SIDE - 1, SIDE))

    loads = [
        pltpu.make_async_copy(source, to, load_sem.at[k])
        for k, (source, to) in enumerate(
            (
                (counts_hbm, counts_flat),
                (block_hbm, block_ref),
                (start_hbm, start_ref),
                (sizes_hbm, sizes_ref),
                (mask_hbm, mask_ref),
                (expr_ref, expr.at[0]),
            )
        )
    ]
    for load in loads:
        load.start()
    barrier = pltpu.get_barrier_semaphore()
    pl.semaphore_signal(barrier, inc=1, device_id={"samples": other}, device_id_type=MESH)

    @pl.when(core == 1)
    def _():
        pl.semaphore_signal(
            barrier, inc=1, device_id={"genes": nxt, "samples": 0}, device_id_type=MESH
        )

    @pl.loop(1, n)
    def _(step):
        pl.semaphore_signal(
            barrier, inc=1, device_id={"genes": mod(me + step, n)}, device_id_type=MESH
        )

    mine = pltpu.make_async_copy(
        dose_ref.at[pl.ds(pl.multiple_of(core * HALF, HALF), HALF)], dose.at[0], local_sem
    )
    mine.start()

    def chunk(i):
        half = lax.shift_right_logical(i + 1, 1)
        return jnp.where((i & 1) == 1, half, mod(SIDE - half, SIDE))

    def message(owner, kind, dest, send, recv):
        return pltpu.make_async_remote_copy(
            src_ref=msgs.at[owner],
            dst_ref=raw.at[kind, me],
            send_sem=sent_sem.at[send],
            recv_sem=recv,
            device_id={"genes": dest},
            device_id_type=MESH,
        )

    def send_chunk(dx):
        row = mod(x + dx, SIDE) * SIDE
        for delta in range(SIDE):
            owner = row + mod(y + delta, SIDE)
            after = mod(owner + 1, n)
            near = delta < SIDE // 2
            kind, dest, twin = (0, owner, after) if near else (1, after, owner)
            give = message(owner, kind, dest, 0, direct_sem.at[kind, dx])
            if delta in (0, SIDE - 1):

                @pl.when(dest != me)
                def _():
                    give.start()

                @pl.when(dest == me)
                def _():
                    pltpu.make_async_copy(
                        msgs.at[owner], raw.at[kind, me], direct_sem.at[kind, dx]
                    ).start()

            else:
                give.start()
            if delta in (1, SIDE - 2):

                @pl.when(y == SIDE - 1 - delta)
                def _():
                    message(owner, 1 - kind, twin, 2, relay_sem.at[1 - kind, dx]).start()

    for load in loads:
        load.wait()
    with jax.named_scope("permute"):
        for t in range(counts_flat.shape[1] // ALIGN):
            counts_ref[t] = counts_flat[:, t * ALIGN : (t + 1) * ALIGN]
        counts_ref[counts_ref.shape[0] - 1] = counts_flat[:, :ALIGN]

        @pl.loop(0, n, unroll=8)
        def _(owner):
            permuted(counts_ref, block_ref, msgs, owner)

    with jax.named_scope("barrier"):
        pl.semaphore_wait(barrier, n + 1 - core)
    expr_copy = pltpu.make_async_remote_copy(
        src_ref=expr_ref,
        dst_ref=expr.at[1],
        send_sem=expr_sem.at[0],
        recv_sem=expr_sem.at[1],
        device_id={"genes": nxt},
        device_id_type=MESH,
    )
    expr_copy.start()
    with jax.named_scope("send"):

        @pl.loop(0, SIDE)
        def _(i):
            send_chunk(chunk(i))

    dose_copy = pltpu.make_async_remote_copy(
        src_ref=dose_ref.at[pl.ds(pl.multiple_of(other * HALF, HALF), HALF)],
        dst_ref=dose.at[1],
        send_sem=dose_sem.at[0],
        recv_sem=dose_sem.at[1],
        device_id={"samples": other},
        device_id_type=MESH,
    )
    dose_copy.start()
    with jax.named_scope("keys"):
        for kind, owner in enumerate((me, prv)):
            membership(sizes_ref, mask_ref, owner, sd.at[kind])
    mine.wait()

    def dose_squares(slot, first, rows):
        for r in range(rows // ALIGN):
            at = pl.ds(pl.multiple_of(first + r * ALIGN, ALIGN), ALIGN)
            square = jnp.zeros((ALIGN, ALIGN), jnp.float32) if slot == 0 else squares[at]
            for k in range(HALF // ALIGN):
                value = dose[slot, at, k * ALIGN : (k + 1) * ALIGN].astype(jnp.float32)
                square = square + value * value
            squares[at] = square

    def column(kind, dx):
        return mod((x if kind == 0 else xp) + SIDE - dx, SIDE)

    def relay_chunk(dx):
        for kind in range(2):
            pltpu.make_async_copy(
                raw.at[kind, 0 : SIDE // 2], raw.at[kind, 0 : SIDE // 2], direct_sem.at[kind, dx]
            ).wait()
        for kind, partner in ((0, nxt), (1, prv)):
            xs = column(kind, dx)

            def send_on(t, sem):
                ys = mod(y + SIDE - t, SIDE) if kind == 0 else mod(y + t, SIDE)
                source = xs * SIDE + ys
                pltpu.make_async_remote_copy(
                    src_ref=raw.at[kind, source],
                    dst_ref=raw.at[1 - kind, source],
                    send_sem=sent_sem.at[sem],
                    recv_sem=relay_sem.at[1 - kind, dx],
                    device_id={"genes": partner},
                    device_id_type=MESH,
                ).start()

            for t in (0, 2, 3):
                send_on(t, 1)

            @pl.when(y != (SIDE - 1 if kind == 0 else 0))
            def _():
                send_on(1, 3 + kind)

    def slots_of(kind, xs):
        at = pl.ds(xs * SIDE, SIDE)
        low = raw[kind, at, :16].reshape(ALIGN, ALIGN)
        high = raw[kind, at, 16:32].reshape(ALIGN, ALIGN)
        left = raw[kind, at, 32:].astype(jnp.float32)
        right = pltpu.roll(left, ALIGN // 2, 2)
        last = jnp.concatenate([left, right], axis=1).reshape(ALIGN, ALIGN).astype(jnp.bfloat16)
        return jnp.concatenate([low, high, last], axis=1)

    def ratio_pair(p):
        pair = (chunk(2 * p), chunk(2 * p + 1))
        for dx in pair:
            for kind in range(2):
                part = raw.at[kind, 0 : SIDE // 2]
                pltpu.make_async_copy(part, part, relay_sem.at[kind, dx]).wait()
        for kind in range(2):
            columns = [column(kind, dx) for dx in pair]
            counts = jnp.concatenate([slots_of(kind, xs) for xs in columns], axis=0)
            both = lax.dot_general(sd[kind], counts, NT, preferred_element_type=jnp.float32)
            ratio = both[RATIOS:] / jnp.maximum(both[:RATIOS], 1.0)
            rest = jnp.ones((ROWS - USED, ALIGN), jnp.float32)
            for k, xs in enumerate(columns):
                own = expr[kind, :, pl.ds(pl.multiple_of(xs * ALIGN, ALIGN), ALIGN)].astype(jnp.float32)
                part = ratio[:, k * ALIGN : (k + 1) * ALIGN]
                panel[kind, 0, xs] = jnp.concatenate([own, part, rest], axis=0).astype(jnp.bfloat16)

    def panel_copy(kind, dx):
        xs = column(kind, dx)
        return pltpu.make_async_remote_copy(
            src_ref=panel.at[kind, 0, xs],
            dst_ref=panel.at[kind, 1, xs],
            send_sem=panel_sem.at[kind, 0],
            recv_sem=panel_sem.at[kind, 1],
            device_id={"samples": other},
            device_id_type=MESH,
        )

    def panel_chunk(dx):
        @pl.when(core == 1)
        def _():
            panel_copy(1, dx).start()

        panel_copy(0, dx).start()

    def pass_on(i, slot=None):
        if slot is not None:
            with jax.named_scope("squares"):
                dose_squares(slot, i * STEP, STEP)
        with jax.named_scope("relay"):
            relay_chunk(chunk(i))

    @pl.loop(0, SIDE // 2)
    def _(i):
        pass_on(i, 0)

    with jax.named_scope("dose_wait"):
        dose_copy.wait_recv()

    @pl.loop(SIDE // 2, SIDE)
    def _(i):
        with jax.named_scope("squares_1"):
            dose_squares(1, (i - SIDE // 2) * STEP, STEP)
        pass_on(i)

    expr_copy.wait()
    count = float(2 * HALF)
    with jax.named_scope("square_rows"):
        for c in range(HALF // 512):
            at = slice(c * 512, (c + 1) * 512)
            stat[:, at] = lax.dot_general(
                jnp.ones((8, ALIGN), jnp.float32),
                squares[at],
                NT,
                precision=lax.Precision.HIGHEST,
                preferred_element_type=jnp.float32,
            )

    def pair_out(p):
        panel_chunk(chunk(2 * p))
        panel_chunk(chunk(2 * p + 1))

    with jax.named_scope("ratio"):
        ratio_pair(0)
    for p in range(1, SIDE // 2):
        with jax.named_scope("ratio_end"):
            ratio_pair(p)
        pair_out(p - 1)

    def joined(kind, slot):
        return jnp.concatenate([panel[kind, slot, k] for k in range(SIDE)], axis=1)

    pair_out(SIDE // 2 - 1)

    PIECE = 48

    def pheno_sums(kind, slot):
        for g in range(ROWS // PIECE):
            rows = slice(g * PIECE, (g + 1) * PIECE)
            total = jnp.zeros((PIECE, ALIGN), jnp.float32) if slot == 0 else pstat[0, rows]
            square = jnp.zeros((PIECE, ALIGN), jnp.float32) if slot == 0 else pstat[1, rows]
            for k in range(SIDE):
                value = panel[kind, slot, k, rows].astype(jnp.float32)
                total = total + value
                square = square + value * value
            if slot == 1:
                total = jnp.sum(total, axis=1, keepdims=True)
                square = jnp.sum(square, axis=1, keepdims=True)
                square = lax.rsqrt(jnp.maximum(square - total * total / count, 1.0))
            pstat[0, rows] = jnp.broadcast_to(total, (PIECE, ALIGN))
            pstat[1, rows] = jnp.broadcast_to(square, (PIECE, ALIGN))

    pheno_sums(1 - core, 0)

    def panel_wait(kind, way):
        pltpu.make_async_copy(panel.at[kind, 1], panel.at[kind, 1], panel_sem.at[kind, way]).wait()

    def assoc(kind, to_ref, scale, after=None):
        left = joined(kind, 1)
        base = joined(kind, 0)

        step = STEP if after is None else ALIGN

        @pl.loop(0, HALF // step)
        def _(c):
            at = pl.multiple_of(c * step, step)
            product = lax.dot_general(
                left, dose[1, pl.ds(at, step)], NT, preferred_element_type=jnp.float32
            )
            if after is not None:

                @pl.when(c > 0)
                def _():
                    after(c - 1)

            product = product + lax.dot_general(
                base, dose[0, pl.ds(at, step)], NT, preferred_element_type=jnp.float32
            )
            for k in range(step // ALIGN):
                tile = c * (step // ALIGN) + k
                here = pl.ds(pl.multiple_of(at + k * ALIGN, ALIGN), ALIGN)
                part = product[:, k * ALIGN : (k + 1) * ALIGN]
                total = part[USED : USED + 1]
                mean = total * (1.0 / count)
                dev = lax.rsqrt(jnp.maximum(stat[0:1, here] - total * mean, 1.0)) * scale
                part = (part - pstat[0] * mean) * dev * pstat[1]
                to_ref[tile] = part.astype(jnp.bfloat16)
        if after is not None:
            after(HALF // step - 1)

    keep = jnp.where(me == 0, 0.0, 1.0)

    first_half, second_half = z_ref.at[0:SIDE], z_ref.at[SIDE : 2 * SIDE]

    def give(c):
        return pltpu.make_async_remote_copy(
            src_ref=back.at[c],
            dst_ref=land.at[c],
            send_sem=back_send_sem,
            recv_sem=back_sem.at[c],
            device_id={"genes": prv, "samples": 1},
            device_id_type=MESH,
        )

    whole = pltpu.make_async_remote_copy(
        src_ref=first_half,
        dst_ref=second_half,
        send_sem=whole_sem.at[0],
        recv_sem=whole_sem.at[1],
        device_id={"samples": 0},
        device_id_type=MESH,
    )

    @pl.when(core == 0)
    def _():
        with jax.named_scope("panel_wait"):
            panel_wait(1, 1)
        with jax.named_scope("pstats_a"):
            pheno_sums(1, 1)
        with jax.named_scope("assoc_a"):
            assoc(1, back, keep, lambda c: give(c).start())
        with jax.named_scope("assoc_b"):
            panel_wait(0, 1)
            pheno_sums(0, 0)
            pheno_sums(0, 1)
            assoc(0, first_half, 1.0)
            whole.wait_recv()

    @pl.when(core == 1)
    def _():
        with jax.named_scope("panel_wait"):
            panel_wait(0, 1)
        with jax.named_scope("pstats_b"):
            pheno_sums(0, 1)
        with jax.named_scope("assoc_c"):
            assoc(0, first_half, 1.0)
            whole.start()

    gene = lax.broadcasted_iota(jnp.int32, (ROWS, ALIGN), 0) & (GENE_DEV - 1)

    def write(m):
        to = pl.ds(pl.multiple_of(m * ALIGN, ALIGN), ALIGN)
        return pltpu.make_async_copy(result.at[m], out_ref.at[:, :, to], out_sem.at[m])

    with jax.named_scope("cut"):

        @pl.loop(0, SIDE)
        def _(m):
            @pl.when(core == 1)
            def _():
                pltpu.make_async_copy(land.at[m], land.at[m], back_sem.at[m]).wait()
                z_ref[SIDE + m] = land[m]

            part = None
            for g in range(GENE_DEV):
                value = z_ref[lax.shift_right_logical(start_ref[g], 7) + m]
                part = value if g == 0 else jnp.where(gene == g, value, part)
            result[m] = part[:USED].reshape(PHEN, GENE_DEV, ALIGN)

            @pl.when(m > 0)
            def _():
                write(m - 1).start()

        write(SIDE - 1).start()
        for m in range(SIDE):
            write(m).wait()

    @pl.when(core == 0)
    def _():
        pltpu.make_async_copy(back, back, back_send_sem).wait()

    dose_copy.wait_send()
    pltpu.make_async_copy(raw.at[0, 0 : n - 2], raw.at[0, 0 : n - 2], sent_sem.at[0]).wait()
    most = raw.at[0, 0 : n - 2 * SIDE]
    pltpu.make_async_copy(most, most, sent_sem.at[1]).wait()
    for sem, there in ((2, inside), (3, y != SIDE - 1), (4, y != 0)):

        @pl.when(there)
        def _():
            few = raw.at[0, 0:SIDE]
            pltpu.make_async_copy(few, few, sent_sem.at[sem]).wait()

    panel_wait(0, 0)

    @pl.when(core == 1)
    def _():
        whole.wait_send()
        panel_wait(1, 0)


def finish(in_ref, out_ref, held, in_sem, out_sem):
    pieces = held.shape[0]
    rows = in_ref.shape[0]
    most = held.shape[1]
    spans = [(k * most, min(most, rows - k * most)) for k in range(pieces)]
    takes = [
        pltpu.make_async_copy(in_ref.at[at : at + size], held.at[k, 0:size], in_sem.at[k])
        for k, (at, size) in enumerate(spans)
    ]
    gives = [
        pltpu.make_async_copy(held.at[k, 0:size], out_ref.at[at : at + size], out_sem.at[k])
        for k, (at, size) in enumerate(spans)
    ]
    for take in takes:
        take.start()
    for take, give in zip(takes, gives):
        take.wait()
        give.start()
    for give in gives:
        give.wait()


def shards(dosage, expression, intron_counts, cluster_sizes, valid_mask, gene_block, window_start):
    n = lax.axis_size("genes")
    dma = pltpu.SemaphoreType.DMA
    bf16, f32 = jnp.bfloat16, jnp.float32
    out = pl.pallas_call(
        functools.partial(kernel, n),
        out_shape=jax.ShapeDtypeStruct((PHEN, GENE_DEV, HALF), bf16),
        in_specs=[pl.BlockSpec(memory_space=pl.ANY)] * 7,
        out_specs=pl.BlockSpec(memory_space=pl.ANY),
        scratch_shapes=[
            pltpu.SMEM(gene_block.shape, jnp.int32),
            pltpu.SMEM(window_start.shape, jnp.int32),
            pltpu.VMEM(cluster_sizes.shape[::-1], jnp.int32),
            pltpu.VMEM(valid_mask.shape[::-1], jnp.int32),
            pltpu.VMEM((2 * SIDE, ROWS, ALIGN), bf16),
            pltpu.VMEM(intron_counts.shape, bf16),
            pltpu.VMEM((intron_counts.shape[1] // ALIGN + 1, 16, ALIGN), bf16),
            pltpu.VMEM((n, SLOTS, ALIGN), bf16),
            pltpu.VMEM((2, n, SLOTS, ALIGN), bf16),
            pltpu.VMEM((2, GENE_DEV, HALF), bf16),
            pltpu.VMEM((2, 2, SIDE, ROWS, ALIGN), bf16),
            pltpu.VMEM((2, HALF, HALF), bf16),
            pltpu.VMEM((HALF, ALIGN), f32),
            pltpu.VMEM((8, HALF), f32),
            pltpu.VMEM((2, ROWS, ALIGN), f32),
            pltpu.VMEM((2, 2 * RATIOS, LANES), bf16),
            pltpu.VMEM((SIDE, ROWS, ALIGN), bf16),
            pltpu.VMEM((SIDE, ROWS, ALIGN), bf16),
            pltpu.VMEM((SIDE, PHEN, GENE_DEV, ALIGN), bf16),
            dma((2, SIDE)),
            dma((2, SIDE)),
            dma((2, 2)),
            dma((5,)),
            dma,
            dma((2,)),
            dma((2,)),
            dma((SIDE,)),
            dma,
            dma((SIDE,)),
            dma((6,)),
            dma((2,)),
        ],
        compiler_params=pltpu.CompilerParams(collective_id=0, has_side_effects=True),
        name="associate",
    )(
        gene_block,
        window_start,
        intron_counts,
        expression,
        cluster_sizes.T,
        valid_mask.T,
        dosage,
    )
    pieces, most = 4, -(-PHEN // 4)
    out = pl.pallas_call(
        finish,
        out_shape=jax.ShapeDtypeStruct(out.shape, out.dtype),
        in_specs=[pl.BlockSpec(memory_space=pl.ANY)],
        out_specs=pl.BlockSpec(memory_space=pl.ANY),
        scratch_shapes=[pltpu.VMEM((pieces, most, GENE_DEV, HALF), bf16), dma((pieces,)), dma((pieces,))],
        name="finish",
    )(out)
    return jnp.swapaxes(out, 0, 1)


def solution(mesh):
    in_specs = (
        P(("parts", "genes"), "samples"),
        P(("parts", "genes"), "samples"),
        P(("parts", "samples", "genes"), None),
        P("parts", None),
        P("parts", None),
        P("parts"),
        P(("parts", "genes")),
    )
    out_specs = P(("parts", "genes"), None, "samples")
    return jax.shard_map(shards, mesh=mesh, in_specs=in_specs, out_specs=out_specs, check_vma=False)
```
